128 devices in a mesh: rep: 1, dp: 128 (over x, y, z, core).
Axes of the slice: x: 4, y: 4, z: 4, core: 2. Of those that a mesh axis runs over, the one named last changes fastest.
Arguments:
- x: bfloat16 [128, 2048, 1024], P(('rep', 'dp'))
- dy: bfloat16 [128, 2048, 1024], P(('rep', 'dp'))
- w_gate: bfloat16 [2, 1024, 2560], P(None, 'dp')
- w_up: bfloat16 [2, 1024, 2560], P(None, 'dp')
- w_down: bfloat16 [2, 2560, 1024], P(None, 'dp')
Outputs:
- output 1: bfloat16 [128, 2048, 1024], P(('rep', 'dp'))
- output 2: bfloat16 [2, 1024, 2560], P('rep', 'dp')
- output 3: bfloat16 [2, 1024, 2560], P('rep', 'dp')
- output 4: bfloat16 [2, 2560, 1024], P('rep', 'dp')
All inputs are finite; a program needn't handle non-finite values.
Results may differ from the reference program's by a relative error of at most 0.018.
Values are sent between devices in bfloat16 or wider.
A program may use at most 1.5 GiB of HBM per device.

```python
import jax
import jax.numpy as jnp
from jax import lax

SEQUENCES = 128
TOKENS = 2048
D = 1024
FF = 2560
LAYERS = 2
NAMES = ("w_gate", "w_up", "w_down")
SHAPES = {"w_gate": (LAYERS, D, FF), "w_up": (LAYERS, D, FF), "w_down": (LAYERS, FF, D)}


def bump(key, n, height):
    away = (jnp.arange(n, dtype=jnp.int32) - jax.random.randint(key, (), 0, n, jnp.int32)) % n
    return jnp.where(away < n // 8, height, 1.0)


def together(key, own, strength):
    shared = jax.random.normal(key, own.shape[1:], jnp.float32)
    return (own + strength * shared) * lax.rsqrt(1 + strength * strength)


def setup_inputs(seed: int = 0, part: int = 0) -> dict:
    kx, kdy, ka, kb, kz, kf, kh, kl, *kw = jax.random.split(jax.random.key(seed), 8 + len(NAMES))
    kx, kdy, ka, kb = (jax.random.fold_in(k, part) for k in (kx, kdy, ka, kb))
    shape = (SEQUENCES, TOKENS, D)
    much_x, much_dy = jax.random.uniform(kz, (2,), jnp.float32, 0.0, 1.0)
    layers = 2.0 ** jax.random.uniform(kl, (LAYERS, 1, 1), jnp.float32, -1.0, 1.0)
    x = together(ka, jax.random.normal(kx, shape, jnp.float32), much_x) * bump(kf, D, 4.0)
    dy = together(kb, jax.random.normal(kdy, shape, jnp.float32), much_dy)
    drawn = {"x": x.astype(jnp.bfloat16), "dy": (dy * (SEQUENCES * TOKENS) ** -0.5).astype(jnp.bfloat16)}
    for key, name in zip(kw, NAMES, strict=True):
        w = jax.random.normal(key, SHAPES[name], jnp.float32) * SHAPES[name][1] ** -0.5
        drawn[name] = (w * {"w_gate": 1.0, "w_up": bump(kh, FF, 4.0), "w_down": layers}[name]).astype(jnp.bfloat16)
    return drawn


def matmul(a, w):
    return jnp.dot(a, w, preferred_element_type=jnp.float32).astype(jnp.bfloat16)


def normed(h):
    wide = h.astype(jnp.float32)
    scale = lax.rsqrt(jnp.mean(wide**2, -1, keepdims=True) + 1e-6)
    return (wide * scale).astype(jnp.bfloat16)


def layer(h, w):
    a = normed(h)
    gate = jnp.dot(a, w["w_gate"], preferred_element_type=jnp.float32)
    up = jnp.dot(a, w["w_up"], preferred_element_type=jnp.float32)
    return h + matmul((jax.nn.silu(gate) * up).astype(jnp.bfloat16), w["w_down"])


def stack(weights, h):
    return lax.scan(lambda h, w: (layer(h, w), None), h, weights)[0]


def reference(x, dy, w_gate, w_up, w_down):
    weights = dict(zip(NAMES, (w_gate, w_up, w_down), strict=True))

    def take(so_far, sequence):
        h, by_y = sequence
        _, back = jax.vjp(stack, weights, h)
        by_weights, by_h = back(by_y)
        return jax.tree.map(lambda total, term: total + term.astype(jnp.float32), so_far, by_weights), by_h

    none_yet = {name: jnp.zeros(w.shape, jnp.float32) for name, w in weights.items()}
    by_weights, by_x = lax.scan(take, none_yet, (x, dy))
    return (by_x, *(by_weights[name].astype(jnp.bfloat16) for name in NAMES))
```

```python
import functools
import jax, jax.numpy as jnp
from jax import lax
from jax.experimental import pallas as pl
from jax.experimental.pallas import tpu as pltpu
from jax.sharding import PartitionSpec as P
T, D, FF, NT, FT = 2048, 1024, 2560, 5, 512
MB = 512
LANES = 128
f32, bf16 = jnp.float32, jnp.bfloat16
def dot(a, b): return jnp.dot(a, b, preferred_element_type=f32)
def dot_t(a, b): return lax.dot_general(a, b, (((1,), (1,)), ((), ())), preferred_element_type=f32)

def norm_into(h_ref, a_ref, rows=256):
    @pl.loop(0, T // rows)
    def _(i):
        r = pl.ds(pl.multiple_of(i * rows, rows), rows)
        w = h_ref[r, :].astype(f32)
        s = lax.rsqrt(jnp.mean(w * w, -1, keepdims=True) + 1e-6)
        a_ref[r, :] = (w * s).astype(bf16)

def fwd0_kernel(base, x_ref, wg_hbm, wu_hbm, wd_hbm, h1_ref, g_hbm, u_hbm, at_hbm,
                a, act, wg, wu, wd, gbuf, ubuf, atbuf, wsem, dsem, osem):
    def wcopy(t, s):
        return (pltpu.make_async_copy(wg_hbm.at[base * NT + t], wg.at[s], wsem.at[0, s]),
                pltpu.make_async_copy(wu_hbm.at[base * NT + t], wu.at[s], wsem.at[1, s]))
    dcopies = [pltpu.make_async_copy(wd_hbm.at[base * 4 + j // 2, j % 2], wd.at[:, pl.ds(LANES * j, LANES)], dsem.at[j]) for j in range(8)]
    for c in wcopy(0, 0): c.start()
    for c in dcopies: c.start()
    norm_into(x_ref, a)
    def ocopy(t, m, s):
        r = pl.ds(pl.multiple_of(m * MB, MB), MB)
        return (pltpu.make_async_copy(gbuf.at[s], g_hbm.at[t, r], osem.at[0, s]),
                pltpu.make_async_copy(ubuf.at[s], u_hbm.at[t, r], osem.at[1, s]),
                pltpu.make_async_copy(atbuf.at[s], at_hbm.at[t, :, r], osem.at[2, s]))
    NM = T // MB
    @pl.loop(0, NT * NM)
    def _(i):
        t = i // NM; m = i % NM; s = t % 2; o = i % 2
        @pl.when(m == 0)
        def _():
            for c in wcopy(t, s): c.wait()
            @pl.when(t + 1 < NT)
            def _():
                for c in wcopy(t + 1, 1 - s): c.start()
        @pl.when(i >= 2)
        def _():
            for c in ocopy(t, m, o): c.wait()
        r = pl.ds(pl.multiple_of(m * MB, MB), MB)
        am = a[r, :]
        g = dot(am, wg[s]); u = dot(am, wu[s])
        gbuf[o] = g; ubuf[o] = u
        ac = (g * jax.nn.sigmoid(g) * u).astype(bf16)
        act[t, r, :] = ac
        atbuf[o] = ac.T
        for c in ocopy(t, m, o): c.start()
    for c in dcopies: c.wait()
    @pl.loop(0, NM)
    def _(m):
        r = pl.ds(pl.multiple_of(m * MB, MB), MB)
        acc = dot(act[0, r, :], wd[0:FT, :])
        for t in range(1, NT):
            acc += dot(act[t, r, :], wd[t * FT:(t + 1) * FT, :])
        h1_ref[r, :] = (x_ref[r, :].astype(f32) + acc.astype(bf16).astype(f32)).astype(bf16)
    for i in (NT * NM - 2, NT * NM - 1):
        for c in ocopy(i // NM, i % NM, i % 2): c.wait()

ANY = pl.BlockSpec(memory_space=pl.ANY)
VM = pl.BlockSpec(memory_space=pltpu.VMEM)
def fwd0(x, wg, wu, wd):
    return pl.pallas_call(
        functools.partial(fwd0_kernel, 0), name="fwd0",
        out_shape=[jax.ShapeDtypeStruct((T, D), bf16), jax.ShapeDtypeStruct((NT, T, FT), f32), jax.ShapeDtypeStruct((NT, T, FT), f32), jax.ShapeDtypeStruct((NT, FT, T), bf16)],
        in_specs=[VM, ANY, ANY, ANY], out_specs=[VM, ANY, ANY, ANY],
        scratch_shapes=[pltpu.VMEM((T, D), bf16), pltpu.VMEM((NT, T, FT), bf16), pltpu.VMEM((2, D, FT), bf16), pltpu.VMEM((2, D, FT), bf16), pltpu.VMEM((FF, D), bf16),
                        pltpu.VMEM((2, MB, FT), f32), pltpu.VMEM((2, MB, FT), f32), pltpu.VMEM((2, FT, MB), bf16),
                        pltpu.SemaphoreType.DMA((2, 2)), pltpu.SemaphoreType.DMA((8,)), pltpu.SemaphoreType.DMA((3, 2))],
        compiler_params=pltpu.CompilerParams(vmem_limit_bytes=60 << 20),
    )(x, wg, wu, wd)

def dact_part(g, u, da):
    s = jax.nn.sigmoid(g)
    p = g * s
    return (da * u * (s + p * (1 - s))).astype(bf16), (da * p).astype(bf16), p

def norm_back(h, da, dh):
    w = h.astype(f32)
    s = lax.rsqrt(jnp.mean(w * w, -1, keepdims=True) + 1e-6)
    d = da.astype(bf16).astype(f32)
    c = jnp.sum(d * w, -1, keepdims=True) * (s * s * s / D)
    return (dh.astype(f32) + (d * s - w * c).astype(bf16).astype(f32)).astype(bf16)

def bwd_kernel(first, *refs):
    base = int(first)
    if first:
        (h_ref, dh_ref, wg_hbm, wu_hbm, wd_hbm, dx_ref, dwg_hbm, dwu_hbm, dwd_hbm,
         a, at, acc, dg, du, wg, wu, wd, ob, actt, dob, wsem, osem, asem, dsem) = refs
    else:
        (h_ref, dh_ref, g_hbm, u_hbm, at_hbm, wg_hbm, wu_hbm, wd_hbm, dx_ref, dwg_hbm, dwu_hbm, dwd_hbm,
         a, at, acc, dg, du, wg, wu, wd, ob, actt, dob, gb, ub, wsem, osem, asem, dsem, gsem) = refs
    NM = T // MB
    def wcopy(t, s):
        tt = pl.ds(t * FT, FT) if isinstance(t, int) else pl.ds(pl.multiple_of(t * FT, FT), FT)
        return [pltpu.make_async_copy(wg_hbm.at[base * NT + t], wg.at[s], wsem.at[0, s]),
                pltpu.make_async_copy(wu_hbm.at[base * NT + t], wu.at[s], wsem.at[1, s])] + [
                pltpu.make_async_copy(wd_hbm.at[base * 4 + j // 2, j % 2, tt], wd.at[s, :, pl.ds(LANES * j, LANES)], wsem.at[2 + j, s]) for j in range(8)]
    def gcopy(i, s):
        t = i // NM; m = i % NM
        r = pl.ds(m * MB if isinstance(m, int) else pl.multiple_of(m * MB, MB), MB)
        return [pltpu.make_async_copy(g_hbm.at[t, r], gb.at[s], gsem.at[0, s]), pltpu.make_async_copy(u_hbm.at[t, r], ub.at[s], gsem.at[1, s])]
    def ocopy(t, s):
        return [pltpu.make_async_copy(ob.at[s, 0], dwg_hbm.at[t], osem.at[0, s]), pltpu.make_async_copy(ob.at[s, 1], dwu_hbm.at[t], osem.at[1, s])]
    for c in wcopy(0, 0): c.start()
    if not first:
        for c in gcopy(0, 0): c.start()
        for t in range(NT): pltpu.make_async_copy(at_hbm.at[t], actt.at[t], asem.at[t]).start()
    rows = 256
    @pl.loop(0, T // rows)
    def _(i):
        r = pl.ds(pl.multiple_of(i * rows, rows), rows)
        w = h_ref[r, :].astype(f32)
        s = lax.rsqrt(jnp.mean(w * w, -1, keepdims=True) + 1e-6)
        av = (w * s).astype(bf16)
        if first: a[r, :] = av
        at[:, r] = av.T
    @pl.loop(0, NT)
    def _(t):
        s = t % 2
        for c in wcopy(t, s): c.wait()
        @pl.when(t + 1 < NT)
        def _():
            for c in wcopy(t + 1, 1 - s): c.start()
        @pl.loop(0, NM)
        def _(m):
            r = pl.ds(pl.multiple_of(m * MB, MB), MB)
            i = t * NM + m
            if first:
                am = a[r, :]
                g = dot(am, wg[s]); u = dot(am, wu[s])
            else:
                o = i % 2
                for c in gcopy(i, o): c.wait()
                @pl.when(i + 1 < NT * NM)
                def _():
                    for c in gcopy(i + 1, 1 - o): c.start()
                g = gb[o]; u = ub[o]
            da = dot_t(dh_ref[r, :], wd[s]).astype(bf16).astype(f32)
            dgv, duv, p = dact_part(g, u, da)
            dg[r, :] = dgv; du[r, :] = duv
            if first: actt[t, :, r] = (p * u).astype(bf16).T
            v = dot_t(dgv, wg[s]) + dot_t(duv, wu[s])
            @pl.when(t == 0)
            def _(): acc[r, :] = v
            @pl.when(t > 0)
            def _(): acc[r, :] += v
        @pl.when(t >= 2)
        def _():
            for c in ocopy(t, s): c.wait()
        @pl.loop(0, D // 512)
        def _(k):
            r = pl.ds(pl.multiple_of(k * 512, 512), 512)
            ob[s, 0, r, :] = dot(at[r, :], dg[...]).astype(bf16)
            ob[s, 1, r, :] = dot(at[r, :], du[...]).astype(bf16)
        for c in ocopy(t, s): c.start()
    @pl.loop(0, NM)
    def _(m):
        r = pl.ds(pl.multiple_of(m * MB, MB), MB)
        dx_ref[r, :] = norm_back(h_ref[r, :], acc[r, :], dh_ref[r, :])
    if not first:
        for t in range(NT): pltpu.make_async_copy(at_hbm.at[t], actt.at[t], asem.at[t]).wait()
    def dcopy(q, s):
        return [pltpu.make_async_copy(dob.at[s, j], dwd_hbm.at[q, j], dsem.at[j, s]) for j in range(2)]
    for q in range(4):
        s = q % 2
        if q >= 2:
            for c in dcopy(q - 2, s): c.wait()
        @pl.loop(0, NT)
        def _(t):
            v = dot(actt[t], dh_ref[:, 256 * q:256 * q + 256]).astype(bf16)
            r = pl.ds(pl.multiple_of(t * FT, FT), FT)
            dob[s, 0, r, :] = v[:, :LANES]
            dob[s, 1, r, :] = v[:, LANES:]
        for c in dcopy(q, s): c.start()
    for q in (2, 3):
        for c in dcopy(q, q % 2): c.wait()
    for t in (NT - 2, NT - 1):
        for c in ocopy(t, t % 2): c.wait()

def bwd(first, h, dh, *rest):
    n = len(rest)
    scr = [pltpu.VMEM((T, D) if first else (16, LANES), bf16), pltpu.VMEM((D, T), bf16), pltpu.VMEM((T, D), f32), pltpu.VMEM((T, FT), bf16), pltpu.VMEM((T, FT), bf16),
           pltpu.VMEM((2, D, FT), bf16), pltpu.VMEM((2, D, FT), bf16), pltpu.VMEM((2, FT, D), bf16), pltpu.VMEM((2, 2, D, FT), bf16),
           pltpu.VMEM((NT, FT, T), bf16), pltpu.VMEM((2, 2, FF, LANES), bf16)]
    if not first: scr += [pltpu.VMEM((2, MB, FT), f32)] * 2
    scr += [pltpu.SemaphoreType.DMA((10, 2)), pltpu.SemaphoreType.DMA((2, 2)), pltpu.SemaphoreType.DMA((NT,)), pltpu.SemaphoreType.DMA((2, 2))]
    if not first: scr += [pltpu.SemaphoreType.DMA((2, 2))]
    return pl.pallas_call(
        functools.partial(bwd_kernel, first), name="bwd1" if first else "bwd0",
        out_shape=[jax.ShapeDtypeStruct((T, D), bf16), jax.ShapeDtypeStruct((NT, D, FT), bf16), jax.ShapeDtypeStruct((NT, D, FT), bf16), jax.ShapeDtypeStruct((4, 2, FF, LANES), bf16)],
        in_specs=[VM, VM] + [ANY] * n, out_specs=[VM, ANY, ANY, ANY],
        scratch_shapes=scr, compiler_params=pltpu.CompilerParams(vmem_limit_bytes=64 * 2**20 - 2**16),
    )(h, dh, *rest)


def compute(x, dy, wg, wu, wd):
    h1, g0, u0, at0 = fwd0(x, wg, wu, wd)
    dh1, *dw1 = bwd(True, h1, dy, wg, wu, wd)
    dx, *dw0 = bwd(False, x, dh1, g0, u0, at0, wg, wu, wd)
    return dx, dw0, dw1

STRIDE = {"x": 32, "y": 8, "z": 2}
AXES = ("x", "y", "z")
ORDER = (("x", "y", "z"), ("y", "z", "x"), ("z", "x", "y"))
LEFT, RIGHT = 3, 1

class Place:
    def __init__(self):
        me = lax.axis_index("dp")
        self.me = me
        self.core = me % 2
        self.at = {"x": me // 32, "y": me // 8 % 4, "z": me // 2 % 4}
    def ring(self, axis, d):
        return (self.at[axis] + d) % 4
    def near(self, axis, d):
        return {"dp": self.me + (self.ring(axis, d) - self.at[axis]) * STRIDE[axis]}
    def partner(self):
        return {"dp": self.me + 1 - 2 * self.core}
    def all(self):
        return [self.partner()] + [self.near(a, d) for a in AXES for d in (LEFT, RIGHT)]

def enter(place):
    barrier = pltpu.get_barrier_semaphore()
    for other in place.all():
        pl.semaphore_signal(barrier, inc=1, device_id=other)
    pl.semaphore_wait(barrier, 7)

def remote(src, dst, send, recv, to):
    return pltpu.make_async_remote_copy(src_ref=src, dst_ref=dst, send_sem=send, recv_sem=recv, device_id=to)

def mult(x, n):
    return x if isinstance(x, int) else pl.multiple_of(x, n)

class Gather:
    STAGES = 8
    def __init__(self, place, ins, outs, send, recv, local):
        self.p, self.ins, self.outs, self.send, self.recv, self.local = place, ins, outs, send, recv, local
    def own(self, c, q):
        if c < 2:
            return self.ins[c].at[q // 5, :, pl.ds(mult(q % 5 * 512, 512), 512)]
        return self.ins[2].at[q // 4, :, pl.ds(mult(q % 4 * 256 + self.p.core * LANES, LANES), LANES)]
    def part(self, c, q, phase, r, half=None, own=False):
        o = ORDER[c]
        pos = {a: slice(None) if j < phase else (r if j == phase else self.p.at[a]) for j, a in enumerate(o)}
        rows = cols = slice(None)
        if half is not None:
            if phase > 0:
                pos[o[0]] = pl.ds(2 * half, 2)
            elif c < 2:
                cols = pl.ds(256 * half, 256)
            else:
                rows = pl.ds(24 * half, 16 if half else 24)
        i = tuple(pos[a] for a in AXES)
        out = self.outs[c]
        return out.at[(q, *i, self.p.core, rows, cols)] if c < 2 else out.at[(q, self.p.core, *i, rows, cols)]
    def sem(self, q, c, k):
        return self.send.at[q, c, k], self.recv.at[q, c, k]
    def copies(self, s, c, q):
        p = self.p
        if s == 6:
            half = self.outs[c].at[q, :, :, :, p.core] if c < 2 else self.outs[c].at[q, p.core]
            return [remote(half, half, *self.sem(q, c, 12), p.partner())]
        phase = s // 2
        a = ORDER[c][phase]
        here = p.at[a]
        k = 4 * phase + 2 * (s % 2)
        if s % 2 == 0:
            dst = self.part(c, q, phase, here)
            src = self.own(c, q) if s == 0 else dst
            return [remote(src, dst, *self.sem(q, c, k), p.near(a, RIGHT)), remote(src, dst, *self.sem(q, c, k + 1), p.near(a, LEFT))]
        l, r = self.part(c, q, phase, p.ring(a, LEFT), 0), self.part(c, q, phase, p.ring(a, RIGHT), 1)
        return [remote(l, l, *self.sem(q, c, k), p.near(a, RIGHT)), remote(r, r, *self.sem(q, c, k + 1), p.near(a, LEFT))]
    def keep(self, c, q):
        return pltpu.make_async_copy(self.own(c, q), self.part(c, q, 0, self.p.at[ORDER[c][0]]), self.local.at[q, c])
    def stage(self, s, c, q):
        if s > 0:
            for x in self.copies(s - 1, c, q): x.wait()
        if s == 0:
            self.keep(c, q).start()
        if s == 2:
            self.keep(c, q).wait()
        if s < 7:
            for x in self.copies(s, c, q): x.start()

def join_down(place, w_in, peer, chip, sem):
    x = remote(w_in, peer, sem.at[0], sem.at[1], place.partner())
    x.start(); x.wait()
    first = place.core == 0
    mine, other = w_in[...].astype(f32), peer[...].astype(f32)
    top, bottom = jnp.where(first, mine, other), jnp.where(first, other, mine)
    chip[...] = jnp.concatenate([top, bottom], axis=1).astype(bf16)

def gather_kernel(wg, wu, wd, og, ou, od, peer, chip, send, recv, local, jsem):
    place = Place()
    enter(place)
    join_down(place, wd, peer, chip, jsem)
    g = Gather(place, (wg, wu, chip), (og, ou, od), send, recv, local)
    @pl.loop(0, 2 * 9 + 8)
    def _(i):
        for s in reversed(range(8)):
            q = (i - s) // 2
            ok = (i >= s) & ((i - s) % 2 == 0) & (q < 10)
            @pl.when(ok)
            def _():
                for c in (0, 1): g.stage(s, c, q)
            @pl.when(ok & (q % 5 < 4))
            def _():
                g.stage(s, 2, q // 5 * 4 + q % 5)

VM = pl.BlockSpec(memory_space=pltpu.VMEM)
ANY = pl.BlockSpec(memory_space=pl.ANY)
def gather(wg, wu, wd):
    return pl.pallas_call(
        gather_kernel, name="gather",
        out_shape=[jax.ShapeDtypeStruct((10, 4, 4, 4, 2, 8, 512), bf16)] * 2 + [jax.ShapeDtypeStruct((8, 2, 4, 4, 4, 40, LANES), bf16)],
        in_specs=[VM] * 3, out_specs=[ANY] * 3,
        scratch_shapes=[pltpu.VMEM((2, 20, 1024), bf16), pltpu.VMEM((2, 40, 1024), bf16),
                        pltpu.SemaphoreType.DMA((10, 3, 13)), pltpu.SemaphoreType.DMA((10, 3, 13)), pltpu.SemaphoreType.DMA((10, 3)), pltpu.SemaphoreType.DMA((2,))],
        compiler_params=pltpu.CompilerParams(collective_id=0, has_side_effects=True, vmem_limit_bytes=60 << 20),
    )(wg, wu, wd)

def parts_shape(c, phase):
    o = ORDER[c]
    n = {a: 4 if j < phase else (2 if j == phase else 1) for j, a in enumerate(o)}
    return tuple(n[a] for a in AXES) + ((8, 512) if c < 2 else (40, LANES))

class Scatter:
    STAGES = 9
    def __init__(self, place, tile, sums, halves, wholes, outs, fin, send, recv, credit, osem):
        self.p, self.tile, self.sums, self.halves, self.wholes, self.outs, self.fin = place, tile, sums, halves, wholes, outs, fin
        self.send, self.recv, self.credit, self.osem = send, recv, credit, osem
    def where(self, c, phase, r, half, ring):
        o = ORDER[c]
        pos = {a: slice(None) if j < phase else (r if j == phase else (self.p.at[a] if ring is None else 0)) for j, a in enumerate(o)}
        rows = cols = slice(None)
        if half is not None:
            if phase > 0:
                pos[o[0]] = pl.ds(2 * half, 2)
            elif c < 2:
                cols = pl.ds(256 * half, 256)
            else:
                rows = pl.ds(24 * half, 16 if half else 24)
        return (*(pos[a] for a in AXES), rows, cols)
    def part(self, c, slot, phase, r, half=None):
        return self.sums[c], (slot, *self.where(c, phase, r, half, None))
    def half_of(self, c, slot, phase, d):
        return self.halves[c][phase], (slot, *self.where(c, phase, d, d, 0))
    def whole_of(self, c, slot, phase, d):
        return self.wholes[c][phase], (slot, *self.where(c, phase, d, None, 0))
    def sem(self, slot, c, k):
        return self.send.at[slot, c, k], self.recv.at[slot, c, k]
    def copies(self, s, c, q, slot):
        p = self.p
        at = lambda x: x[0].at[x[1]]
        if s == 0:
            t = self.tile(c, slot)
            src = t.at[:, :, :, 1 - p.core] if c < 2 else t.at[1 - p.core]
            return [remote(src, self.sums[c].at[slot], *self.sem(slot, c, 12), p.partner())]
        if s == 7:
            fin = at(self.part(c, slot, 0, p.at[ORDER[c][0]]))
            if c < 2:
                return [pltpu.make_async_copy(fin, self.outs[c].at[q // 5, :, pl.ds(mult(q % 5 * 512, 512), 512)], self.osem.at[slot, c])]
            return [remote(fin, self.fin.at[q // 4, :, pl.ds(mult(q % 4 * 256 + p.core * LANES, LANES), LANES)], *self.sem(slot, c, 13), p.partner())]
        phase = 2 - (s - 1) // 2
        a = ORDER[c][phase]
        k = 4 * phase + 2 * ((s - 1) % 2)
        if s % 2 == 1:
            two = [(at(self.part(c, slot, phase, p.ring(a, 2), d)), at(self.half_of(c, slot, phase, d))) for d in (0, 1)]
        else:
            two = [(at(self.part(c, slot, phase, p.ring(a, (RIGHT, LEFT)[d]))), at(self.whole_of(c, slot, phase, d))) for d in (0, 1)]
        return [remote(*two[d], *self.sem(slot, c, k + d), p.near(a, (RIGHT, LEFT)[d])) for d in (0, 1)]
    def add(self, into, *terms):
        ref, i = into
        v = ref[i].astype(f32)
        for r, j in terms: v = v + r[j].astype(f32)
        ref[i] = v.astype(bf16)
    def stage(self, s, c, q, slot, wait_credit=None):
        p = self.p
        if s > 0:
            for x in self.copies(s - 1, c, q, slot): x.wait()
        if s == 0:
            @pl.when(wait_credit)
            def _():
                for i in range(7): pl.semaphore_wait(self.credit.at[c, i], 1)
        elif s == 1:
            t = self.tile(c, slot)
            @pl.loop(0, 4)
            def _(x):
                mine = t[x, :, :, p.core] if c < 2 else t[p.core, x]
                self.sums[c][slot, x] = (mine.astype(f32) + self.sums[c][slot, x].astype(f32)).astype(bf16)
        elif s == 8:
            if c == 2:
                i = (q // 4, slice(None), pl.ds(mult(q % 4 * 256 + p.core * LANES, LANES), LANES))
                ref, j = self.part(c, slot, 0, p.at[ORDER[c][0]])
                self.fin[i] = ref[j]
        else:
            phase = 2 - (s - 2) // 2
            a = ORDER[c][phase]
            if s % 2 == 0:
                for d in (0, 1):
                    self.add(self.part(c, slot, phase, p.ring(a, (RIGHT, LEFT)[d]), d), self.half_of(c, slot, phase, d))
            else:
                self.add(self.part(c, slot, phase, p.at[a]), *(self.whole_of(c, slot, phase, d) for d in (0, 1)))
        if s < 8:
            for x in self.copies(s, c, q, slot): x.start()
    def release(self, c):
        for i, other in enumerate(self.p.all()):
            pl.semaphore_signal(self.credit.at[c, (0, 2, 1, 4, 3, 6, 5)[i]], inc=1, device_id=other)
    def finish_down(self, out):
        first = self.p.core == 0
        v = self.fin[...].astype(f32)
        out[...] = jnp.where(first, v[:, :20], v[:, 20:]).astype(bf16)

def scatter_scratch(slots=2):
    sums = [pltpu.VMEM((slots, 4, 4, 4, 8, 512), bf16)] * 2 + [pltpu.VMEM((slots, 4, 4, 4, 40, LANES), bf16)]
    rings = [pltpu.VMEM((slots, *parts_shape(c, ph)), bf16) for c in range(3) for ph in range(3)]
    return sums + rings * 2 + [pltpu.VMEM((2, 40, 1024), bf16), pltpu.SemaphoreType.DMA((slots, 3, 14)), pltpu.SemaphoreType.DMA((slots, 3, 14)),
                               pltpu.SemaphoreType.REGULAR((3, 7)), pltpu.SemaphoreType.DMA((slots, 2))]

def make_scatter(place, tile, outs, refs):
    sums, halves, wholes = refs[:3], refs[3:12], refs[12:21]
    fin, send, recv, credit, osem = refs[21:26]
    nine = lambda r: [r[3 * c:3 * c + 3] for c in range(3)]
    return Scatter(place, tile, sums, nine(halves), nine(wholes), outs, fin, send, recv, credit, osem)

def scatter_kernel(g0, u0, d0, g1, u1, d1, og, ou, od, tg, tu, td, tsem, *refs):
    place = Place()
    enter(place)
    tiles, hbm = (tg, tu, td), ((g0, u0, d0), (g1, u1, d1))
    sc = make_scatter(place, lambda c, slot: tiles[c].at[slot], (og, ou), refs)
    def load(c, q, slot):
        n = 5 if c < 2 else 4
        for l in (0, 1):
            @pl.when(q // n == l)
            def _():
                x = pltpu.make_async_copy(hbm[l][c].at[q % n], tiles[c].at[slot], tsem.at[slot, c])
                x.start(); x.wait()
    EVERY = 5
    @pl.loop(0, EVERY * 9 + 9)
    def _(i):
        for s in reversed(range(9)):
            q = (i - s) // EVERY
            slot = q % 2
            ok = (i >= s) & ((i - s) % EVERY == 0) & (q < 10)
            def go(c, n, q):
                if s == 0:
                    load(c, q, slot)
                sc.stage(s, c, q, slot, q_all >= 2 if s == 0 else None)
                if s == 8:
                    @pl.when(q_all < n - 2)
                    def _(): sc.release(c)
            q_all = q
            @pl.when(ok)
            def _():
                for c in (0, 1): go(c, 10, q)
            @pl.when(ok & (q < 8))
            def _(): go(2, 8, q)
    sc.finish_down(od)

def scatter(*terms):
    return pl.pallas_call(
        scatter_kernel, name="scatter",
        out_shape=[jax.ShapeDtypeStruct((2, 8, 2560), bf16)] * 2 + [jax.ShapeDtypeStruct((2, 20, 1024), bf16)],
        in_specs=[ANY] * 6, out_specs=[ANY, ANY, VM],
        scratch_shapes=[pltpu.VMEM((2, 4, 4, 4, 2, 8, 512), bf16)] * 2 + [pltpu.VMEM((2, 2, 4, 4, 4, 40, LANES), bf16), pltpu.SemaphoreType.DMA((2, 3))] + scatter_scratch(),
        compiler_params=pltpu.CompilerParams(collective_id=1, has_side_effects=True, vmem_limit_bytes=60 << 20),
    )(*terms)


def solution(mesh):
    def step(x, dy, wg, wu, wd):
        tg, tu, td = gather(wg, wu, wd)
        tg, tu, td = tg.reshape(2 * NT, D, FT), tu.reshape(2 * NT, D, FT), td.reshape(8, 2, FF, LANES)
        dx, dw0, dw1 = compute(x[0], dy[0], tg, tu, td)
        shape = ((NT, 4, 4, 4, 2, 8, 512), (NT, 4, 4, 4, 2, 8, 512), (4, 2, 4, 4, 4, 40, LANES))
        terms = [v.reshape(s) for dw in (dw0, dw1) for v, s in zip(dw, shape)]
        return (dx[None], *scatter(*terms))

    tokens, rows = P(("rep", "dp")), P(None, "dp", None)
    return jax.shard_map(step, mesh=mesh, in_specs=(tokens, tokens, rows, rows, rows), out_specs=(tokens,) + (P("rep", "dp", None),) * 3, check_vma=False)
```

```python
import functools
import jax, jax.numpy as jnp
from jax import lax
from jax.experimental import pallas as pl
from jax.experimental.pallas import tpu as pltpu
from jax.sharding import PartitionSpec as P

f32, bf16 = jnp.float32, jnp.bfloat16
T, D, FF = 2048, 1024, 2560
NT, FT = 5, 512
NQ, LANES = 4, 128
MB = 512
NM = T // MB
ROWS = FF // 4
AXES = ("x", "y", "z")
STRIDE = {"x": 32, "y": 8, "z": 2}
ORDER = (("x", "y", "z"), ("y", "z", "x"), ("z", "x", "y"))
LEFT, RIGHT, ACROSS = 3, 1, 2
GU, DOWN = (0, 1), 2
CHIPS = (4, 4, 4)
BLOCK = ((8, FT), (8, FT), (40, LANES))
TILE = ((*CHIPS, 2, *BLOCK[0]), (*CHIPS, 2, *BLOCK[1]), (2, *CHIPS, *BLOCK[DOWN]))
NTILES = (NT, NT, NQ)
ALL = slice(None)


def dot(a, b):
    return jnp.dot(a, b, preferred_element_type=f32)


def dot_t(a, b):
    return lax.dot_general(a, b, (((1,), (1,)), ((), ())), preferred_element_type=f32)


def mult(x, n):
    return x if isinstance(x, int) else pl.multiple_of(x, n)


def span(i, n):
    return pl.ds(mult(i * n, n), n)


def normed(h):
    w = h.astype(f32)
    return (w * lax.rsqrt(jnp.mean(w * w, -1, keepdims=True) + 1e-6)).astype(bf16)


def norm_back(h, da, dh):
    w = h.astype(f32)
    s = lax.rsqrt(jnp.mean(w * w, -1, keepdims=True) + 1e-6)
    d = da.astype(bf16).astype(f32)
    c = jnp.sum(d * w, -1, keepdims=True) * (s * s * s / D)
    return (dh.astype(f32) + (d * s - w * c).astype(bf16).astype(f32)).astype(bf16)


class Place:
    def __init__(self):
        self.me = lax.axis_index("dp")
        self.core = self.me % 2
        self.at = {a: self.me // STRIDE[a] % 4 for a in AXES}

    def ring(self, axis, d):
        return (self.at[axis] + d) % 4

    def near(self, axis, d):
        return {"dp": self.me + (self.ring(axis, d) - self.at[axis]) * STRIDE[axis]}

    def partner(self):
        return {"dp": self.me + 1 - 2 * self.core}

    def others(self):
        return [self.partner()] + [self.near(a, d) for a in AXES for d in (LEFT, RIGHT)]

    def enter(self):
        barrier = pltpu.get_barrier_semaphore()
        for other in self.others():
            pl.semaphore_signal(barrier, inc=1, device_id=other)
        pl.semaphore_wait(barrier, 7)


def remote(src, dst, send, recv, to):
    return pltpu.make_async_remote_copy(src_ref=src, dst_ref=dst, send_sem=send, recv_sem=recv, device_id=to)


def where(c, phase, r, half, rest):
    o = ORDER[c]
    pos = {a: ALL if j < phase else (r if j == phase else rest(a)) for j, a in enumerate(o)}
    rows = cols = ALL
    if half is not None:
        if phase > 0:
            pos[o[0]] = pl.ds(2 * half, 2)
        elif c in GU:
            cols = pl.ds(FT // 2 * half, FT // 2)
        else:
            rows = pl.ds(24 * half, 16 if half else 24)
    return (*(pos[a] for a in AXES), rows, cols)


class Gather:
    def __init__(self, place, layer, ins, outs, send, recv, local):
        self.p, self.layer, self.ins, self.outs, self.send, self.recv, self.local = place, layer, ins, outs, send, recv, local

    def own(self, c, q):
        if c in GU:
            return self.ins[c], (self.layer, ALL, span(q, FT))
        return self.ins[c], (self.layer, ALL, span(q * 2 + self.p.core, LANES))

    def index(self, c, q, phase, r, half=None):
        i = where(c, phase, r, half, lambda a: self.p.at[a])
        return (q, *i[:3], self.p.core, *i[3:]) if c in GU else (q, self.p.core, *i)

    def copies(self, s, c, q):
        p, out = self.p, self.outs[c]
        sem = lambda k: (self.send.at[self.layer, q, c, k], self.recv.at[self.layer, q, c, k])
        if s == 6:
            half = out.at[q, :, :, :, p.core] if c in GU else out.at[q, p.core]
            return [remote(half, half, *sem(2 * s), p.partner())]
        phase = s // 2
        a = ORDER[c][phase]
        if s % 2 == 0:
            dst = out.at[self.index(c, q, phase, p.at[a])]
            ref, i = self.own(c, q)
            two = [(ref.at[i] if s == 0 else dst, dst)] * 2
        else:
            two = [(out.at[self.index(c, q, phase, p.ring(a, d), h)],) * 2 for h, d in enumerate((LEFT, RIGHT))]
        return [remote(*two[h], *sem(2 * s + h), p.near(a, d)) for h, d in enumerate((RIGHT, LEFT))]

    def keep(self, c, q):
        ref, i = self.own(c, q)
        return ref, i, self.outs[c], self.index(c, q, 0, self.p.at[ORDER[c][0]])

    def stage(self, s, c, q):
        if s > 0:
            for x in self.copies(s - 1, c, q): x.wait()
        if self.local is None:
            if s == 0:
                ref, i, out, j = self.keep(c, q)
                out[j] = ref[i]
        elif s in (0, 2):
            ref, i, out, j = self.keep(c, q)
            x = pltpu.make_async_copy(ref.at[i], out.at[j], self.local.at[q, c])
            x.wait() if s else x.start()
        if s < 7:
            for x in self.copies(s, c, q): x.start()


def join_down(place, w_in, peer, chip):
    first = place.core == 0
    mine, other = w_in[...].astype(f32), peer[...].astype(f32)
    chip[...] = jnp.concatenate([jnp.where(first, mine, other), jnp.where(first, other, mine)], axis=1).astype(bf16)


def fwd_kernel(x_ref, wg_in, wu_in, wd_in, h1_ref, g_hbm, u_hbm, at_hbm, wg0, wu0, wd0, wg1, wu1, wd1,
               a, act, tg, tu, td, wd, gb, ub, atb, peer, chip, send, recv, local, jsem, wsem, dsem, osem):
    place = Place()
    place.enter()
    join = remote(wd_in, peer, jsem.at[0], jsem.at[1], place.partner())
    join.start()
    ins = (wg_in, wu_in, chip)
    layers = [Gather(place, 0, ins, (tg, tu, td), send, recv, None), Gather(place, 1, ins, (wg1, wu1, wd1), send, recv, local)]

    def tick(i):
        for s in reversed(range(8)):
            for l in (1, 0):
                q = i - s - NT * l
                @pl.when((q >= 0) & (q < NT))
                def _():
                    for c in GU: layers[l].stage(s, c, q)
                if s == 0 and l == 0:
                    @pl.when(i == 0)
                    def _():
                        join.wait()
                        join_down(place, wd_in, peer, chip)
                @pl.when((q >= 0) & (q < NQ))
                def _():
                    layers[l].stage(s, DOWN, q)

    rows = T // 8
    @pl.loop(0, 8)
    def _(i):
        tick(i)
        a[span(i, rows), :] = normed(x_ref[span(i, rows), :])

    def kept(t):
        return [pltpu.make_async_copy(v.at[t], o.at[t], wsem.at[t, c]) for c, (v, o) in enumerate(((tg, wg0), (tu, wu0)))]
    def kept_down(q):
        return pltpu.make_async_copy(td.at[q], wd0.at[q], wsem.at[q, DOWN])
    def down(j):
        return pltpu.make_async_copy(wd0.at[j // 2, j % 2], wd.at[:, :, :, :, span(j, LANES)], dsem.at[j])
    def out(t, m, s):
        r = span(m, MB)
        return [pltpu.make_async_copy(gb.at[s], g_hbm.at[t, r], osem.at[0, s]),
                pltpu.make_async_copy(ub.at[s], u_hbm.at[t, r], osem.at[1, s]),
                pltpu.make_async_copy(atb.at[s], at_hbm.at[span(t, FT), r], osem.at[2, s])]

    @pl.loop(0, NT * NM)
    def _(i):
        t, m = i // NM, i % NM
        o = i % 2
        @pl.when(m == 0)
        def _():
            for x in kept(t): x.start()
            @pl.when(t == 3)
            def _():
                for q in range(NQ): kept_down(q).start()
            @pl.when(t == 4)
            def _():
                for q in range(NQ): kept_down(q).wait()
                for j in range(2 * NQ): down(j).start()
        @pl.when(i >= 2)
        def _():
            for x in out(t, m, o): x.wait()
        am = a[span(m, MB), :]
        g = dot(am, tg[t].reshape(D, FT))
        u = dot(am, tu[t].reshape(D, FT))
        gb[o] = g
        ub[o] = u
        ac = (g * jax.nn.sigmoid(g) * u).astype(bf16)
        act[span(m, MB), span(t, FT)] = ac
        atb[o] = ac.T
        for x in out(t, m, o): x.start()
        @pl.when(m == 2)
        def _():
            tick(8 + t)

    for j in range(2 * NQ): down(j).wait()
    @pl.loop(0, NM)
    def _(m):
        r = span(m, MB)
        acc = dot(act[r, :], wd[...].reshape(FF, D))
        h1_ref[r, :] = (x_ref[r, :].astype(f32) + acc.astype(bf16).astype(f32)).astype(bf16)
        tick(8 + NT + m)
    for i in (NT * NM - 2, NT * NM - 1):
        for x in out(i // NM, i % NM, i % 2): x.wait()
    for t in range(NT):
        for x in kept(t): x.wait()


VM = pl.BlockSpec(memory_space=pltpu.VMEM)
ANY = pl.BlockSpec(memory_space=pl.ANY)
DMA = pltpu.SemaphoreType.DMA


def of(dtype, *shape):
    return jax.ShapeDtypeStruct(shape, dtype)


def vm(*shape, dtype=bf16):
    return pltpu.VMEM(shape, dtype)


def forward(x, *weights):
    tiles = [of(bf16, n, *tile) for n, tile in zip(NTILES, TILE)]
    return pl.pallas_call(
        fwd_kernel, name="fwd",
        out_shape=[of(bf16, T, D), of(f32, NT, T, FT), of(f32, NT, T, FT), of(bf16, FF, T)] + tiles * 2,
        in_specs=[VM] * 4, out_specs=[VM] + [ANY] * 9,
        scratch_shapes=[vm(T, D), vm(T, FF)] + [vm(n, *tile) for n, tile in zip(NTILES, TILE)] + [
            vm(*CHIPS, 40, D), vm(2, MB, FT, dtype=f32), vm(2, MB, FT, dtype=f32), vm(2, FT, MB), vm(2, 20, D), vm(2, 40, D),
            DMA((2, NT, 3, 13)), DMA((2, NT, 3, 13)), DMA((NT, 3)), DMA((2,)), DMA((NT, 3)), DMA((2 * NQ,)), DMA((3, 2))],
        compiler_params=pltpu.CompilerParams(collective_id=0, has_side_effects=True, vmem_limit_bytes=63 << 20),
    )(x, *weights)


class Scatter:
    def __init__(self, place, c, slots, total, tile, out, sums, halves, wholes, send, recv, credit, osem=None, fin=None):
        self.p, self.c, self.slots, self.total, self.tile, self.out, self.sums = place, c, slots, total, tile, out, sums
        self.halves, self.wholes, self.send, self.recv, self.credit, self.osem, self.fin = halves, wholes, send, recv, credit, osem, fin

    def part(self, n, phase, r, half=None):
        return self.sums, (n, *where(self.c, phase, r, half, lambda a: self.p.at[a]))

    def got(self, bufs, n, phase, d, half=None):
        return bufs[phase], (n, *where(self.c, phase, d, None if phase else half, lambda a: 0))

    def final(self, q, core):
        n = NTILES[self.c]
        return (1 - q // n, ALL, span(q % n, FT) if self.c in GU else span(q % n * 2 + core, LANES))

    def copies(self, s, q):
        p, c, n = self.p, self.c, q % self.slots
        at = lambda x: x[0].at[x[1]]
        sem = lambda k: (self.send.at[n, k], self.recv.at[n, k])
        if s == 0:
            t = self.tile(q)
            return [remote(t.at[:, :, :, 1 - p.core] if c in GU else t.at[1 - p.core], self.sums.at[n], *sem(0), p.partner())]
        if s == 7:
            end = at(self.part(n, 0, p.at[ORDER[c][0]]))
            if c in GU:
                return [pltpu.make_async_copy(end, self.out.at[self.final(q, 0)], self.osem.at[n])]
            return [remote(end, self.fin.at[self.final(q, p.core)], *sem(1), p.partner())]
        phase = 2 - (s - 1) // 2
        a = ORDER[c][phase]
        ways = (RIGHT, LEFT)
        if s % 2:
            two = [(self.part(n, phase, p.ring(a, ACROSS), d), self.got(self.halves, n, phase, d, d)) for d in (0, 1)]
        else:
            two = [(self.part(n, phase, p.ring(a, ways[d])), self.got(self.wholes, n, phase, d)) for d in (0, 1)]
        return [remote(at(two[d][0]), at(two[d][1]), *sem(2 * s + d), p.near(a, ways[d])) for d in (0, 1)]

    def add(self, into, *terms):
        ref, i = into
        v = ref[i].astype(f32)
        for r, j in terms: v = v + r[j].astype(f32)
        ref[i] = v.astype(bf16)

    def stage(self, s, q):
        p, c, n = self.p, self.c, q % self.slots
        if s > 0:
            for x in self.copies(s - 1, q): x.wait()
        if s == 0:
            @pl.when(q >= self.slots)
            def _():
                for i in range(7): pl.semaphore_wait(self.credit.at[i], 1)
        elif s == 1:
            t = self.tile(q)
            @pl.loop(0, 4)
            def _(x):
                mine = t[x, :, :, p.core] if c in GU else t[p.core, x]
                self.sums[n, x] = (mine.astype(f32) + self.sums[n, x].astype(f32)).astype(bf16)
        elif s == 8:
            if c == DOWN:
                ref, j = self.part(n, 0, p.at[ORDER[c][0]])
                self.fin[self.final(q, p.core)] = ref[j]
            @pl.when(q < self.total - self.slots)
            def _():
                for i, other in enumerate(p.others()):
                    pl.semaphore_signal(self.credit.at[(0, 2, 1, 4, 3, 6, 5)[i]], inc=1, device_id=other)
        else:
            phase = 2 - (s - 2) // 2
            a = ORDER[c][phase]
            if s % 2 == 0:
                for d, way in enumerate((RIGHT, LEFT)):
                    self.add(self.part(n, phase, p.ring(a, way), d), self.got(self.halves, n, phase, d, d))
            else:
                self.add(self.part(n, phase, p.at[a]), *(self.got(self.wholes, n, phase, d) for d in (0, 1)))
        if s < 8:
            for x in self.copies(s, q): x.start()


def ring_shape(c, phase, half):
    n = {a: 4 if j < phase else (2 if j == phase else 1) for j, a in enumerate(ORDER[c])}
    if half and phase:
        n[ORDER[c][0]] = 2
    return tuple(n[a] for a in AXES) + BLOCK[c]


SLOTS = (2, 2, 3)
STEP = 6
FIRST, LATER = (1, 3, 5, 6), (1, 2, 3, 4)
EVERY, DOWN_AT = 3, (0, 1, 2, 4, 5, 6, 7, 8, 9)
DOWN1, DOWN0, LAST = 5, 8, 12


def bwd_kernel(h_hbm, dy_hbm, x_hbm, g_hbm, u_hbm, at_hbm, wg0, wu0, wd0, wg1, wu1, wd1,
               dx_hbm, at1_hbm, og, ou, od,
               a, dh, at, acc, dg, du, wg, wu, wd, ob, dob, actt, gb, ub, atb,
               wsem, gsem, bsem, dsem, xsem, *refs):
    place = Place()
    place.enter()
    refs = list(refs)
    take = lambda n: [refs.pop(0) for _ in range(n)]
    fin, = take(1)
    tiles = (lambda q: ob.at[q % 2, 0], lambda q: ob.at[q % 2, 1], lambda q: dob.at[q % NQ])
    outs = (og, ou, None)
    sc = []
    for c in range(3):
        sums, = take(1)
        sc.append(Scatter(place, c, SLOTS[c], 2 * NTILES[c], tiles[c], outs[c], sums, take(3), take(3), *take(4), fin))

    def weights(f, s):
        for l, (g_, u_, d_) in enumerate(((wg1, wu1, wd1), (wg0, wu0, wd0))):
            yield f // NT == l, [pltpu.make_async_copy(g_.at[f % NT], wg.at[s], wsem.at[0, s]), pltpu.make_async_copy(u_.at[f % NT], wu.at[s], wsem.at[1, s])] + [
                pltpu.make_async_copy(d_.at[j // 2, j % 2, span(f % NT, FT)], wd.at[s, :, span(j, LANES)], wsem.at[2 + j, s]) for j in range(2 * NQ)]
    def saved(t, m, s):
        return [pltpu.make_async_copy(g_hbm.at[t, span(m, MB)], gb.at[s], gsem.at[0, s]), pltpu.make_async_copy(u_hbm.at[t, span(m, MB)], ub.at[s], gsem.at[1, s])]
    def act_out(t, m):
        return pltpu.make_async_copy(atb, at1_hbm.at[span(t, FT), span(m, MB)], bsem)
    def act_in(src, t):
        return pltpu.make_async_copy(src.at[span(t, ROWS)], actt.at[t % 2], dsem.at[t % 2])
    def dx_out(m):
        return pltpu.make_async_copy(dh.at[span(m, MB)], dx_hbm.at[span(m, MB)], xsem.at[m])

    load_h, load_dy, load_x = (pltpu.make_async_copy(src, dst, xsem.at[i]) for i, (src, dst) in enumerate(((h_hbm, a), (dy_hbm, dh), (x_hbm, a))))
    loads = (load_h, load_dy)
    for x in loads: x.start()
    for x in next(weights(0, 0))[1]: x.start()
    for x in loads: x.wait()

    rows = 256
    @pl.loop(0, T // rows)
    def _(i):
        v = normed(a[span(i, rows), :])
        a[span(i, rows), :] = v
        at[:, span(i, rows)] = v.T

    def ff_block(layer, f, s, m):
        t, r = f % NT, span(m, MB)
        o = m % 2
        if layer:
            am = a[r, :]
            g, u = dot(am, wg[s]), dot(am, wu[s])
        else:
            for x in saved(t, m, o): x.wait()
            i = t * NM + m + 1
            @pl.when(i < NT * NM)
            def _():
                for x in saved(i // NM, i % NM, 1 - o): x.start()
            g, u = gb[o], ub[o]
        d = dot_t(dh[r, :], wd[s]).astype(bf16).astype(f32)
        sg = jax.nn.sigmoid(g)
        p = g * sg
        dgv = (d * u * (sg + p * (1 - sg))).astype(bf16)
        duv = (d * p).astype(bf16)
        dg[r, :] = dgv
        du[r, :] = duv
        if layer:
            @pl.when(f * NM + m > 0)
            def _():
                act_out(t, m).wait()
            atb[...] = (p * u).astype(bf16).T
            act_out(t, m).start()
        v = dot_t(dgv, wg[s]) + dot_t(duv, wu[s])
        @pl.when(t == 0)
        def _(): acc[r, :] = v
        @pl.when(t > 0)
        def _(): acc[r, :] += v

    def tick(S, j):
        def gate_up(s, back):
            S0 = S - back
            @pl.when((S0 >= 0) & (S0 < LAST) & (S0 != DOWN1) & (S0 != DOWN0))
            def _():
                q = S0 - (S0 > DOWN1).astype(jnp.int32) - (S0 > DOWN0).astype(jnp.int32)
                for c in GU: sc[c].stage(s, q)
        for k, i in enumerate(LATER):
            if j == i - 1: gate_up(1 + len(FIRST) + k, 2)
        for k, i in enumerate(FIRST):
            if j == i - 1: gate_up(1 + k, 1)
        if j == STEP - 1: gate_up(0, 0)
        @pl.when(S > DOWN1)
        def _():
            for s in reversed(range(9)):
                if (j - DOWN_AT[s]) % EVERY == 0:
                    for l, start in ((1, DOWN1 + 1), (0, DOWN0 + 1)):
                        d = (STEP * (S - start) + j - DOWN_AT[s]) // EVERY
                        @pl.when((d >= 0) & (d < NQ))
                        def _(): sc[DOWN].stage(s, d + NQ * (1 - l))

    @pl.loop(0, STEP * (LAST + 2))
    def _(i):
        S, j = i // STEP, i % STEP
        is_down = (S == DOWN1) | (S == DOWN0)
        is_ff = (S < LAST) & (S != DOWN1) & (S != DOWN0)
        f = S - (S > DOWN1).astype(jnp.int32) - (S > DOWN0).astype(jnp.int32)
        s = f % 2
        @pl.when(is_ff & (j == 0))
        def _():
            for ok, copies in weights(f, s):
                @pl.when(ok)
                def _():
                    for x in copies: x.wait()
            for ok, copies in weights(f + 1, 1 - s):
                @pl.when(ok & (f + 1 < 2 * NT))
                def _():
                    for x in copies: x.start()
        @pl.when((S < DOWN1) & (j < NM))
        def _():
            ff_block(1, f, s, j)
        @pl.when(is_ff & (S > DOWN1) & (j < NM))
        def _():
            ff_block(0, f, s, j)
        @pl.when(is_ff & (j >= NM))
        def _():
            r, x = span(j - NM, MB), pl.ds(2 * (j - NM), 2)
            for c, v in ((0, dg), (1, du)):
                ob[s, c, x] = dot(at[r, :], v[...]).reshape(2, *TILE[c][1:]).astype(bf16)
        @pl.when(is_down)
        def _():
            @pl.when(j == 0)
            def _():
                @pl.when(S == DOWN1)
                def _():
                    act_out(NT - 1, NM - 1).wait()
                    load_h.start()
                    act_in(at1_hbm, 0).start()
                    for x in saved(0, 0, 0): x.start()
                @pl.when(S == DOWN0)
                def _():
                    act_in(at_hbm, 0).start()
            @pl.when(j < 4)
            def _():
                act_in(at_hbm, j).wait()
                @pl.when((j < 3) & (S == DOWN1))
                def _(): act_in(at1_hbm, j + 1).start()
                @pl.when((j < 3) & (S == DOWN0))
                def _(): act_in(at_hbm, j + 1).start()
                v = dot(actt[j % 2], dh[...])
                for k in range(2 * NQ):
                    dob[k // 2, k % 2, j] = v[:, k * LANES:(k + 1) * LANES].reshape(4, 4, 40, LANES).astype(bf16)
            @pl.when((S == DOWN1) & (j == NT))
            def _():
                load_h.wait()
                @pl.loop(0, T // rows)
                def _(i):
                    r = span(i, rows)
                    dh[r, :] = norm_back(a[r, :], acc[r, :], dh[r, :])
                load_x.start()
                load_x.wait()
                @pl.loop(0, T // rows)
                def _(i):
                    at[:, span(i, rows)] = normed(a[span(i, rows), :]).T
        @pl.when((S == LAST) & (j < NM))
        def _():
            r = span(j, MB)
            dh[r, :] = norm_back(a[r, :], acc[r, :], dh[r, :])
            dx_out(j).start()
        for k in range(STEP):
            @pl.when(j == k)
            def _(): tick(S, k)
    first = place.core == 0
    v = fin[...].astype(f32)
    od[...] = jnp.where(first, v[:, :20], v[:, 20:]).astype(bf16)
    for m in range(NM): dx_out(m).wait()


def backward(h1, dy, x, g, u, at, *tiles):
    two = [t.reshape((NT, D, FT) if c in GU else (NQ, 2, FF, LANES)) for t, c in zip(tiles, (0, 1, 2) * 2)]
    rings = []
    for c in range(3):
        rings += [vm(SLOTS[c], *CHIPS, *BLOCK[c])] + [vm(SLOTS[c], *ring_shape(c, ph, half)) for half in (True, False) for ph in range(3)] + [DMA((SLOTS[c], 18)), DMA((SLOTS[c], 18)), pltpu.SemaphoreType.REGULAR((7,)), DMA((SLOTS[c],))]
    return pl.pallas_call(
        bwd_kernel, name="bwd",
        out_shape=[of(bf16, T, D), of(bf16, FF, T), of(bf16, 2, 8, FF), of(bf16, 2, 8, FF), of(bf16, 2, 20, D)],
        in_specs=[ANY] * 12, out_specs=[ANY] * 4 + [VM],
        scratch_shapes=[vm(T, D), vm(T, D), vm(D, T), vm(T, D, dtype=f32), vm(T, FT), vm(T, FT), vm(2, D, FT), vm(2, D, FT), vm(2, FT, D),
                        vm(2, 2, *TILE[0]), vm(NQ, *TILE[DOWN]), vm(2, ROWS, T), vm(2, MB, FT, dtype=f32), vm(2, MB, FT, dtype=f32), vm(FT, MB),
                        DMA((10, 2)), DMA((2, 2)), DMA, DMA((2,)), DMA((NM,)), vm(2, 40, D)] + rings,
        compiler_params=pltpu.CompilerParams(collective_id=1, has_side_effects=True, vmem_limit_bytes=(64 << 20) - (64 << 10)),
    )(h1, dy, x, g, u, at, *two)


def solution(mesh):
    def step(x, dy, *weights):
        h1, g, u, at, *tiles = forward(x[0], *weights)
        dx, _, *grads = backward(h1, dy[0], x[0], g, u, at, *tiles)
        return (dx[None], *grads)

    tokens, rows = P(("rep", "dp")), P(None, "dp", None)
    return jax.shard_map(step, mesh=mesh, in_specs=(tokens, tokens, rows, rows, rows), out_specs=(tokens,) + (P("rep", "dp", None),) * 3, check_vma=False)
```

```python
import functools, itertools
import jax, jax.numpy as jnp
from jax import lax
from jax.experimental import pallas as pl
from jax.experimental.pallas import tpu as pltpu
from jax.sharding import PartitionSpec as P

f32, bf16 = jnp.float32, jnp.bfloat16
T, D, FF = 2048, 1024, 2560
NT, FT = 5, 512
NQ, LANES = 4, 128
MB = 512
SUBS = 1
NM = T // MB
ROWS = FF // 4
AXES = ("x", "y", "z")
STRIDE = {"x": 32, "y": 8, "z": 2}
ORDER = (("x", "y", "z"), ("y", "z", "x"), ("z", "x", "y"))
LEFT, RIGHT, ACROSS = 3, 1, 2
GU, DOWN = (0, 1), 2
CHIPS = (4, 4, 4)
BLOCK = ((8, FT), (8, FT), (40, LANES))
TILE = ((*CHIPS, 2, *BLOCK[0]), (*CHIPS, 2, *BLOCK[1]), (2, *CHIPS, *BLOCK[DOWN]))
NTILES = (NT, NT, NQ)
ALL = slice(None)


def dot(a, b):
    return jnp.dot(a, b, preferred_element_type=f32)


def dot_t(a, b):
    return lax.dot_general(a, b, (((1,), (1,)), ((), ())), preferred_element_type=f32)


def mult(x, n):
    return x if isinstance(x, int) else pl.multiple_of(x, n)


def span(i, n):
    return pl.ds(mult(i * n, n), n)


def normed(h):
    w = h.astype(f32)
    return (w * lax.rsqrt(jnp.mean(w * w, -1, keepdims=True) + 1e-6)).astype(bf16)


def norm_back(h, da, dh):
    w = h.astype(f32)
    s = lax.rsqrt(jnp.mean(w * w, -1, keepdims=True) + 1e-6)
    d = da.astype(bf16).astype(f32)
    c = jnp.sum(d * w, -1, keepdims=True) * (s * s * s / D)
    return (dh.astype(f32) + (d * s - w * c).astype(bf16).astype(f32)).astype(bf16)


class Place:
    def __init__(self):
        self.me = lax.axis_index("dp")
        self.core = self.me % 2
        self.at = {a: self.me // STRIDE[a] % 4 for a in AXES}

    def ring(self, axis, d):
        return (self.at[axis] + d) % 4

    def shifted(self, *moves):
        return {"dp": self.me + sum((self.ring(a, d) - self.at[a]) * STRIDE[a] for a, d in moves)}

    def partner(self):
        return {"dp": self.me + 1 - 2 * self.core}

    def in_plane(self, c, k, way=1):
        return tuple(zip(ORDER[c][:2], (way * (k // 4) % 4, way * (k % 4) % 4)))

    def enter(self):
        barrier = pltpu.get_barrier_semaphore()
        moves = [m for m in itertools.product(range(4), repeat=3) if 0 in m and any(m)]
        for m in moves:
            pl.semaphore_signal(barrier, inc=1, device_id=self.shifted(*zip(AXES, m)))
        pl.semaphore_signal(barrier, inc=1, device_id=self.partner())
        pl.semaphore_wait(barrier, len(moves) + 1)


PEERS = range(1, 16)


def remote(src, dst, send, recv, to):
    return pltpu.make_async_remote_copy(src_ref=src, dst_ref=dst, send_sem=send, recv_sem=recv, device_id=to)


def block(c, place, moves=()):
    pos = dict(moves)
    return tuple(place.ring(a, pos[a]) if a in pos else place.at[a] for a in AXES)


def plane(c, r, half=None):
    o = ORDER[c]
    pos = {o[0]: ALL if half is None else pl.ds(2 * half, 2), o[1]: ALL, o[2]: r}
    return tuple(pos[a] for a in AXES)


def joint(place, buf, sem):
    return remote(buf, buf, *sem, place.partner())


class Gather:
    STAGES = 5

    def __init__(self, place, layer, ins, outs, size, send, recv, local):
        self.p, self.layer, self.ins, self.outs, self.size = place, layer, ins, outs, size
        self.send, self.recv, self.local = send, recv, local

    def own(self, c, q):
        if c in GU:
            return self.ins[c], (self.layer, ALL, span(q, FT))
        return self.ins[c], (self.layer, ALL, span(q * 2 + self.p.core, LANES))

    def index(self, c, q, i):
        return (q, *i, self.p.core) if c in GU else (q, self.p.core, *i)

    def sem(self, c, q, k):
        return self.send.at[self.layer, q, c, k], self.recv.at[self.layer, q, c, k]

    def copies(self, s, c, q):
        p, out = self.p, self.outs[c]
        sem = functools.partial(self.sem, c, q)
        if s == 0:
            ref, i = self.own(c, q)
            return [remote(ref.at[i], out.at[self.index(c, q, block(c, p))], *sem(0), p.shifted(*p.in_plane(c, k))) for k in PEERS]
        if s == 3:
            half = out.at[self.index(c, q, (ALL,) * 3)]
            return [remote(half, half, *sem(5), p.partner())]
        a = ORDER[c][2]
        if s == 1:
            whole = [out.at[self.index(c, q, plane(c, p.at[a]))]] * 2
        else:
            whole = [out.at[self.index(c, q, plane(c, p.ring(a, d), h))] for h, d in enumerate((LEFT, RIGHT))]
        return [remote(whole[h], whole[h], *sem(2 * s - 1 + h), p.shifted((a, d))) for h, d in enumerate((RIGHT, LEFT))]

    def stage(self, s, c, q):
        ref, i = self.own(c, q)
        keep = (self.outs[c], self.index(c, q, block(c, self.p)))
        if s == 1:
            joint(self.p, self.size[c], self.sem(c, q, 0)).wait()
        elif s > 1:
            for x in self.copies(s - 1, c, q): x.wait()
        if self.local is None:
            if s == 0:
                keep[0][keep[1]] = ref[i]
        elif s < 2:
            x = pltpu.make_async_copy(ref.at[i], keep[0].at[keep[1]], self.local.at[q, c])
            x.wait() if s else x.start()
        if s < 4:
            for x in self.copies(s, c, q): x.start()


def join_down(place, w_in, peer, chip):
    first = place.core == 0
    mine, other = w_in[...].astype(f32), peer[...].astype(f32)
    chip[...] = jnp.concatenate([jnp.where(first, mine, other), jnp.where(first, other, mine)], axis=1).astype(bf16)


APART = 2
READY0 = APART * 4


def fwd_kernel(x_ref, wg_in, wu_in, wd_in, h1_ref, g_hbm, u_hbm, at_hbm, wg0, wu0, wd0, wg1, wu1, wd1,
               a, act, tg, tu, td, wd, gb, ub, atb, peer, chip, size_gu, size_down, send, recv, local, jsem, wsem, dsem, osem):
    place = Place()
    place.enter()
    join = remote(wd_in, peer, jsem.at[0], jsem.at[1], place.partner())
    join.start()
    ins = (wg_in, wu_in, chip)
    size = (size_gu, size_gu, size_down)
    layers = [Gather(place, 0, ins, (tg, tu, td), size, send, recv, None), Gather(place, 1, ins, (wg1, wu1, wd1), size, send, recv, local)]

    def tick(i):
        for s in reversed(range(Gather.STAGES)):
            for l in (1, 0):
                q = i - APART * s - NT * l
                @pl.when((q >= 0) & (q < NT))
                def _():
                    for c in GU: layers[l].stage(s, c, q)
                if s == 0 and l == 0:
                    @pl.when(i == 0)
                    def _():
                        join.wait()
                        join_down(place, wd_in, peer, chip)
                @pl.when((q >= 0) & (q < NQ))
                def _():
                    layers[l].stage(s, DOWN, q)

    rows = T // 8
    @pl.loop(0, 8)
    def _(i):
        @pl.when(i <= READY0)
        def _(): tick(i)
        a[span(i, rows), :] = normed(x_ref[span(i, rows), :])
    for i in range(8, READY0 + 1): tick(i)

    def kept(t):
        return [pltpu.make_async_copy(v.at[t], o.at[t], wsem.at[t, c]) for c, (v, o) in enumerate(((tg, wg0), (tu, wu0)))]
    def kept_down(q):
        return pltpu.make_async_copy(td.at[q], wd0.at[q], wsem.at[q, DOWN])
    def down(j):
        return pltpu.make_async_copy(wd0.at[j // 2, j % 2], wd.at[:, :, :, :, span(j, LANES)], dsem.at[j])
    def out(t, m, s):
        r = span(m, MB)
        return [pltpu.make_async_copy(gb.at[s], g_hbm.at[t, r], osem.at[0, s]),
                pltpu.make_async_copy(ub.at[s], u_hbm.at[t, r], osem.at[1, s]),
                pltpu.make_async_copy(atb.at[s], at_hbm.at[span(t, FT), r], osem.at[2, s])]

    @pl.loop(0, NT * NM)
    def _(i):
        t, m = i // NM, i % NM
        o = i % 2
        @pl.when(m == 0)
        def _():
            for x in kept(t): x.start()
            @pl.when(t == 3)
            def _():
                for q in range(NQ): kept_down(q).start()
            @pl.when(t == 4)
            def _():
                for q in range(NQ): kept_down(q).wait()
                for j in range(2 * NQ): down(j).start()
        @pl.when(i >= 2)
        def _():
            for x in out(t, m, o): x.wait()
        am = a[span(m, MB), :]
        g = dot(am, tg[t].reshape(D, FT))
        u = dot(am, tu[t].reshape(D, FT))
        gb[o] = g
        ub[o] = u
        ac = (g * jax.nn.sigmoid(g) * u).astype(bf16)
        act[span(m, MB), span(t, FT)] = ac
        atb[o] = ac.T
        for x in out(t, m, o): x.start()
        @pl.when(m == 2)
        def _():
            tick(READY0 + 1 + t)

    for j in range(2 * NQ): down(j).wait()
    @pl.loop(0, NM)
    def _(m):
        r = span(m, MB)
        acc = dot(act[r, :], wd[...].reshape(FF, D))
        h1_ref[r, :] = (x_ref[r, :].astype(f32) + acc.astype(bf16).astype(f32)).astype(bf16)
        tick(READY0 + 1 + NT + m)
    @pl.loop(READY0 + 1 + NT + NM, READY0 + 2 * NT)
    def _(i):
        tick(i)
    for i in (NT * NM - 2, NT * NM - 1):
        for x in out(i // NM, i % NM, i % 2): x.wait()
    for t in range(NT):
        for x in kept(t): x.wait()


VM = pl.BlockSpec(memory_space=pltpu.VMEM)
ANY = pl.BlockSpec(memory_space=pl.ANY)
DMA = pltpu.SemaphoreType.DMA


def of(dtype, *shape):
    return jax.ShapeDtypeStruct(shape, dtype)


def vm(*shape, dtype=bf16):
    return pltpu.VMEM(shape, dtype)


def forward(x, *weights):
    tiles = [of(bf16, n, *tile) for n, tile in zip(NTILES, TILE)]
    return pl.pallas_call(
        fwd_kernel, name="fwd",
        out_shape=[of(bf16, T, D), of(f32, NT, T, FT), of(f32, NT, T, FT), of(bf16, FF, T)] + tiles * 2,
        in_specs=[VM] * 4, out_specs=[VM] + [ANY] * 9,
        scratch_shapes=[vm(T, D), vm(T, FF)] + [vm(n, *tile) for n, tile in zip(NTILES, TILE)] + [
            vm(*CHIPS, 40, D), vm(2, MB, FT, dtype=f32), vm(2, MB, FT, dtype=f32), vm(2, FT, MB), vm(2, 20, D), vm(2, 40, D), vm(15, *BLOCK[0]), vm(15, *BLOCK[DOWN]),
            DMA((2, NT, 3, 6)), DMA((2, NT, 3, 6)), DMA((NT, 3)), DMA((2,)), DMA((NT, 3)), DMA((2 * NQ,)), DMA((3, 2))],
        compiler_params=pltpu.CompilerParams(collective_id=0, has_side_effects=True, vmem_limit_bytes=63 << 20),
    )(x, *weights)


class Scatter:
    STAGES = 6

    def __init__(self, place, c, slots, total, tile, out, fin, sums, halves, wholes, blocks, send, recv, credit, osem):
        self.p, self.c, self.slots, self.total, self.tile, self.out, self.fin = place, c, slots, total, tile, out, fin
        self.sums, self.halves, self.wholes, self.blocks = sums, halves, wholes, blocks
        self.send, self.recv, self.credit, self.osem = send, recv, credit, osem

    def final(self, q, core):
        n = NTILES[self.c]
        return (1 - q // n, ALL, span(q % n, FT) if self.c in GU else span(q % n * 2 + core, LANES))

    def sem(self, q, k):
        return self.send.at[q % self.slots, k], self.recv.at[q % self.slots, k]

    def copies(self, s, q):
        p, c, n = self.p, self.c, q % self.slots
        sem = functools.partial(self.sem, q)
        if s == 0:
            t = self.tile(q)
            return [remote(t.at[:, :, :, 1 - p.core] if c in GU else t.at[1 - p.core], self.sums.at[n], *sem(0), p.partner())]
        if s == 3:
            ways = [(k, p.in_plane(c, k, -1)) for k in PEERS]
            return [remote(self.sums.at[(n, *block(c, p, m))], self.blocks.at[n, k - 1], *sem(5), p.shifted(*m)) for k, m in ways]
        if s == 4:
            end = self.sums.at[(n, *block(c, p))]
            if c in GU:
                return [pltpu.make_async_copy(end, self.out.at[self.final(q, 0)], self.osem.at[n])]
            return [remote(end, self.fin.at[self.final(q, p.core)], *sem(6), p.partner())]
        a = ORDER[c][2]
        ways = (RIGHT, LEFT)
        if s == 1:
            two = [(self.sums.at[(n, *plane(c, p.ring(a, ACROSS), d))], self.halves.at[n, d]) for d in (0, 1)]
        else:
            two = [(self.sums.at[(n, *plane(c, p.ring(a, ways[d])))], self.wholes.at[n, d]) for d in (0, 1)]
        return [remote(*two[d], *sem(2 * s - 1 + d), p.shifted((a, ways[d]))) for d in (0, 1)]

    def add(self, i, *terms):
        v = self.sums[i].astype(f32)
        for t in terms: v = v + t.astype(f32)
        self.sums[i] = v.astype(bf16)

    def stage(self, s, q):
        p, c, n = self.p, self.c, q % self.slots
        a = ORDER[c][2]
        if s == 4:
            joint(p, self.blocks.at[n], self.sem(q, 5)).wait()
        elif s > 0:
            for x in self.copies(s - 1, q): x.wait()
        if s == 0:
            @pl.when(q >= self.slots)
            def _():
                for i in range(18): pl.semaphore_wait(self.credit.at[i], 1)
        elif s == 1:
            t = self.tile(q)
            @pl.loop(0, 4)
            def _(x):
                self.add((n, x), t[x, :, :, p.core] if c in GU else t[p.core, x])
        elif s == 2:
            for d, way in enumerate((RIGHT, LEFT)):
                self.add((n, *plane(c, p.ring(a, way), d)), self.halves[n, d])
        elif s == 3:
            self.add((n, *plane(c, p.at[a])), self.wholes[n, 0], self.wholes[n, 1])
        elif s == 4:
            self.add((n, *block(c, p)), *(self.blocks[n, k - 1] for k in PEERS))
        else:
            if c == DOWN:
                self.fin[self.final(q, p.core)] = self.sums[(n, *block(c, p))]
            @pl.when(q < self.total - self.slots)
            def _():
                others = [p.partner(), p.shifted((a, LEFT)), p.shifted((a, RIGHT))] + [p.shifted(*p.in_plane(c, k)) for k in PEERS]
                for i, other in enumerate(others):
                    pl.semaphore_signal(self.credit.at[i], inc=1, device_id=other)
        if s < 5:
            for x in self.copies(s, q): x.start()


SLOTS = (2, 2, 3)
STEP = 6
FIRST, LATER = (1, 3, 5), (2, 4)
EVERY, DOWN_AT = 3, (0, 1, 3, 5, 7, 8)
DOWN1, DOWN0, LAST = 5, 8, 12


def bwd_kernel(h_hbm, dy_hbm, x_hbm, g_hbm, u_hbm, at_hbm, wg0, wu0, wd0, wg1, wu1, wd1,
               dx_hbm, at1_hbm, og, ou, od,
               a, dh, at, acc, dg, du, wg, wu, wd, ob, dob, actt, gb, ub, atb,
               wsem, gsem, bsem, dsem, xsem, *refs):
    place = Place()
    place.enter()
    refs = list(refs)
    take = lambda n: [refs.pop(0) for _ in range(n)]
    fin, = take(1)
    tiles = (lambda q: ob.at[q % 2, 0], lambda q: ob.at[q % 2, 1], lambda q: dob.at[q % NQ])
    outs = (og, ou, None)
    sc = []
    for c in range(3):
        sc.append(Scatter(place, c, SLOTS[c], 2 * NTILES[c], tiles[c], outs[c], fin, *take(8)))

    def weights(f, s):
        for l, (g_, u_, d_) in enumerate(((wg1, wu1, wd1), (wg0, wu0, wd0))):
            yield f // NT == l, [pltpu.make_async_copy(g_.at[f % NT], wg.at[s], wsem.at[0, s]), pltpu.make_async_copy(u_.at[f % NT], wu.at[s], wsem.at[1, s])] + [
                pltpu.make_async_copy(d_.at[j // 2, j % 2, span(f % NT, FT)], wd.at[s, :, span(j, LANES)], wsem.at[2 + j, s]) for j in range(2 * NQ)]
    def saved(t, m, s):
        return [pltpu.make_async_copy(g_hbm.at[t, span(m, MB)], gb.at[s], gsem.at[0, s]), pltpu.make_async_copy(u_hbm.at[t, span(m, MB)], ub.at[s], gsem.at[1, s])]
    def act_out(t, m):
        return pltpu.make_async_copy(atb, at1_hbm.at[span(t, FT), span(m, MB)], bsem)
    def act_in(src, t):
        return pltpu.make_async_copy(src.at[span(t, ROWS)], actt.at[t % 2], dsem.at[t % 2])
    def dx_out(m):
        return pltpu.make_async_copy(dh.at[span(m, MB)], dx_hbm.at[span(m, MB)], xsem.at[m])

    load_h, load_dy, load_x = (pltpu.make_async_copy(src, dst, xsem.at[i]) for i, (src, dst) in enumerate(((h_hbm, a), (dy_hbm, dh), (x_hbm, a))))
    loads = (load_h, load_dy)
    for x in loads: x.start()
    for x in next(weights(0, 0))[1]: x.start()
    for x in loads: x.wait()

    rows = 256
    @pl.loop(0, T // rows)
    def _(i):
        v = normed(a[span(i, rows), :])
        a[span(i, rows), :] = v
        at[:, span(i, rows)] = v.T

    def ff_block(layer, f, s, m):
        t, o = f % NT, m % 2
        n = MB // SUBS
        rows = [pl.ds(mult(m * MB + n * k, n), n) for k in range(SUBS)]
        if layer:
            gu = [(dot(a[r, :], wg[s]), dot(a[r, :], wu[s])) for r in rows]
        else:
            for x in saved(t, m, o): x.wait()
            i = t * NM + m + 1
            @pl.when(i < NT * NM)
            def _():
                for x in saved(i // NM, i % NM, 1 - o): x.start()
            gu = [(gb[o, n * k:n * k + n], ub[o, n * k:n * k + n]) for k in range(SUBS)]
        if layer:
            @pl.when(f * NM + m > 0)
            def _():
                act_out(t, m).wait()
        ds = [dot_t(dh[r, :], wd[s]).astype(bf16).astype(f32) for r in rows]
        back = []
        for k, (r, (g, u), d) in enumerate(zip(rows, gu, ds)):
            sg = jax.nn.sigmoid(g)
            p = g * sg
            dgv = (d * u * (sg + p * (1 - sg))).astype(bf16)
            duv = (d * p).astype(bf16)
            dg[r, :] = dgv
            du[r, :] = duv
            if layer:
                atb[:, n * k:n * k + n] = (p * u).astype(bf16).T
            back.append((dgv, duv))
        for r, (dgv, duv) in zip(rows, back):
            acc[r, :] += dot_t(dgv, wg[s]) + dot_t(duv, wu[s])
        if layer:
            act_out(t, m).start()

    def tick(S, j):
        def gate_up(s, back):
            S0 = S - back
            @pl.when((S0 >= 0) & (S0 < LAST) & (S0 != DOWN1) & (S0 != DOWN0))
            def _():
                q = S0 - (S0 > DOWN1).astype(jnp.int32) - (S0 > DOWN0).astype(jnp.int32)
                for c in GU: sc[c].stage(s, q)
        for k, i in enumerate(LATER):
            if j == i: gate_up(1 + len(FIRST) + k, 2)
        for k, i in enumerate(FIRST):
            if j == i: gate_up(1 + k, 1)
        if j == STEP - 1: gate_up(0, 0)
        @pl.when(S > DOWN1)
        def _():
            for s in reversed(range(Scatter.STAGES)):
                if (j - DOWN_AT[s]) % EVERY == 0:
                    for l, start in ((1, DOWN1 + 1), (0, DOWN0 + 1)):
                        d = (STEP * (S - start) + j - DOWN_AT[s]) // EVERY
                        @pl.when((d >= 0) & (d < NQ))
                        def _(): sc[DOWN].stage(s, d + NQ * (1 - l))

    @pl.loop(0, STEP * (LAST + 2))
    def _(i):
        S, j = i // STEP, i % STEP
        is_down = (S == DOWN1) | (S == DOWN0)
        is_ff = (S < LAST) & (S != DOWN1) & (S != DOWN0)
        f = S - (S > DOWN1).astype(jnp.int32) - (S > DOWN0).astype(jnp.int32)
        s = f % 2
        @pl.when(is_ff & (j == 0))
        def _():
            @pl.when(f % NT == 0)
            def _():
                acc[...] = jnp.zeros_like(acc)
            for ok, copies in weights(f, s):
                @pl.when(ok)
                def _():
                    for x in copies: x.wait()
            for ok, copies in weights(f + 1, 1 - s):
                @pl.when(ok & (f + 1 < 2 * NT))
                def _():
                    for x in copies: x.start()
        @pl.when((S < DOWN1) & (j < NM))
        def _():
            ff_block(1, f, s, j)
        @pl.when(is_ff & (S > DOWN1) & (j < NM))
        def _():
            ff_block(0, f, s, j)
        @pl.when(is_ff & (j >= NM))
        def _():
            r, x = span(j - NM, MB), pl.ds(2 * (j - NM), 2)
            for c, v in ((0, dg), (1, du)):
                ob[s, c, x] = dot(at[r, :], v[...]).reshape(2, *TILE[c][1:]).astype(bf16)
        @pl.when(is_down)
        def _():
            @pl.when(j == 0)
            def _():
                @pl.when(S == DOWN1)
                def _():
                    act_out(NT - 1, NM - 1).wait()
                    load_h.start()
                    act_in(at1_hbm, 0).start()
                    for x in saved(0, 0, 0): x.start()
                @pl.when(S == DOWN0)
                def _():
                    act_in(at_hbm, 0).start()
            @pl.when(j < 4)
            def _():
                act_in(at_hbm, j).wait()
                @pl.when((j < 3) & (S == DOWN1))
                def _(): act_in(at1_hbm, j + 1).start()
                @pl.when((j < 3) & (S == DOWN0))
                def _(): act_in(at_hbm, j + 1).start()
                v = dot(actt[j % 2], dh[...])
                for k in range(2 * NQ):
                    dob[k // 2, k % 2, j] = v[:, k * LANES:(k + 1) * LANES].reshape(4, 4, 40, LANES).astype(bf16)
            @pl.when((S == DOWN1) & (j == NT))
            def _():
                load_h.wait()
                @pl.loop(0, T // rows)
                def _(i):
                    r = span(i, rows)
                    dh[r, :] = norm_back(a[r, :], acc[r, :], dh[r, :])
                load_x.start()
                load_x.wait()
                @pl.loop(0, T // rows)
                def _(i):
                    at[:, span(i, rows)] = normed(a[span(i, rows), :]).T
        @pl.when((S == LAST) & (j < NM))
        def _():
            r = span(j, MB)
            dh[r, :] = norm_back(a[r, :], acc[r, :], dh[r, :])
            dx_out(j).start()
        for k in range(STEP):
            @pl.when(j == k)
            def _(): tick(S, k)
    first = place.core == 0
    v = fin[...].astype(f32)
    od[...] = jnp.where(first, v[:, :20], v[:, 20:]).astype(bf16)
    for m in range(NM): dx_out(m).wait()


def backward(h1, dy, x, g, u, at, *tiles):
    two = [t.reshape((NT, D, FT) if c in GU else (NQ, 2, FF, LANES)) for t, c in zip(tiles, (0, 1, 2) * 2)]
    rings = []
    for c in range(3):
        n = SLOTS[c]
        flat = [4 // (1 + (ORDER[c][0] == x)) for x in AXES if x != ORDER[c][2]]
        rings += [vm(n, *CHIPS, *BLOCK[c]), vm(n, 2, *flat, *BLOCK[c]), vm(n, 2, 4, 4, *BLOCK[c]), vm(n, 15, *BLOCK[c]),
                  DMA((n, 7)), DMA((n, 7)), pltpu.SemaphoreType.REGULAR((18,)), DMA((n,))]
    return pl.pallas_call(
        bwd_kernel, name="bwd",
        out_shape=[of(bf16, T, D), of(bf16, FF, T), of(bf16, 2, 8, FF), of(bf16, 2, 8, FF), of(bf16, 2, 20, D)],
        in_specs=[ANY] * 12, out_specs=[ANY] * 4 + [VM],
        scratch_shapes=[vm(T, D), vm(T, D), vm(D, T), vm(T, D, dtype=f32), vm(T, FT), vm(T, FT), vm(2, D, FT), vm(2, D, FT), vm(2, FT, D),
                        vm(2, 2, *TILE[0]), vm(NQ, *TILE[DOWN]), vm(2, ROWS, T), vm(2, MB, FT, dtype=f32), vm(2, MB, FT, dtype=f32), vm(FT, MB),
                        DMA((10, 2)), DMA((2, 2)), DMA, DMA((2,)), DMA((NM,)), vm(2, 40, D)] + rings,
        compiler_params=pltpu.CompilerParams(collective_id=1, has_side_effects=True, vmem_limit_bytes=(64 << 20) - (64 << 10)),
    )(h1, dy, x, g, u, at, *two)


def solution(mesh):
    def step(x, dy, *weights):
        h1, g, u, at, *tiles = forward(x[0], *weights)
        dx, _, *grads = backward(h1, dy[0], x[0], g, u, at, *tiles)
        return (dx[None], *grads)

    tokens, rows = P(("rep", "dp")), P(None, "dp", None)
    return jax.shard_map(step, mesh=mesh, in_specs=(tokens, tokens, rows, rows, rows), out_specs=(tokens,) + (P("rep", "dp", None),) * 3, check_vma=False)
```

```python
import functools, itertools
import jax, jax.numpy as jnp
from jax import lax
from jax.experimental import pallas as pl
from jax.experimental.pallas import tpu as pltpu
from jax.sharding import PartitionSpec as P

f32, bf16 = jnp.float32, jnp.bfloat16
T, D, FF = 2048, 1024, 2560
NT, FT = 5, 512
NQ, LANES = 4, 128
MB = 512
SUBS = 1
NM = T // MB
ROWS = FF // 4
AXES = ("x", "y", "z")
STRIDE = {"x": 32, "y": 8, "z": 2}
ORDER = (("x", "y", "z"), ("y", "z", "x"), ("z", "x", "y"))
LEFT, RIGHT, ACROSS = 3, 1, 2
GU, DOWN = (0, 1), 2
CHIPS = (4, 4, 4)
BLOCK = ((8, FT), (8, FT), (40, LANES))
TILE = ((*CHIPS, 2, *BLOCK[0]), (*CHIPS, 2, *BLOCK[1]), (2, *CHIPS, *BLOCK[DOWN]))
NTILES = (NT, NT, NQ)
VMEM = (64 << 20) - (64 << 10)
ALL = slice(None)


def dot(a, b):
    return jnp.dot(a, b, preferred_element_type=f32)


def dot_t(a, b):
    return lax.dot_general(a, b, (((1,), (1,)), ((), ())), preferred_element_type=f32)


def mult(x, n):
    return x if isinstance(x, int) else pl.multiple_of(x, n)


def span(i, n):
    return pl.ds(mult(i * n, n), n)


def sigmoid(x):
    return 0.5 * jnp.tanh(0.5 * x) + 0.5


def normed(h):
    w = h.astype(f32)
    return (w * lax.rsqrt(jnp.mean(w * w, -1, keepdims=True) + 1e-6)).astype(bf16)


def norm_back(h, da, dh):
    w = h.astype(f32)
    s = lax.rsqrt(jnp.mean(w * w, -1, keepdims=True) + 1e-6)
    d = da.astype(bf16).astype(f32)
    c = jnp.sum(d * w, -1, keepdims=True) * (s * s * s / D)
    return (dh.astype(f32) + (d * s - w * c).astype(bf16).astype(f32)).astype(bf16)


class Place:
    def __init__(self):
        self.me = lax.axis_index("dp")
        self.core = self.me % 2
        self.at = {a: self.me // STRIDE[a] % 4 for a in AXES}

    def ring(self, axis, d):
        return (self.at[axis] + d) % 4

    def shifted(self, *moves):
        return {"dp": self.me + sum((self.ring(a, d) - self.at[a]) * STRIDE[a] for a, d in moves)}

    def partner(self):
        return {"dp": self.me + 1 - 2 * self.core}

    def in_plane(self, c, k, way=1):
        return tuple(zip(ORDER[c][:2], (way * (k // 4) % 4, way * (k % 4) % 4)))

    def enter(self, still):
        barrier = pltpu.get_barrier_semaphore()
        moves = [m for m in itertools.product(range(4), repeat=3) if 3 > m.count(0) >= still]
        for m in moves:
            pl.semaphore_signal(barrier, inc=1, device_id=self.shifted(*zip(AXES, m)))
        pl.semaphore_signal(barrier, inc=1, device_id=self.partner())
        pl.semaphore_wait(barrier, len(moves) + 1)


PEERS = range(1, 16)


def remote(src, dst, send, recv, to):
    return pltpu.make_async_remote_copy(src_ref=src, dst_ref=dst, send_sem=send, recv_sem=recv, device_id=to)


def block(c, place, moves=()):
    pos = dict(moves)
    return tuple(place.ring(a, pos[a]) if a in pos else place.at[a] for a in AXES)


def plane(c, r, half=None):
    o = ORDER[c]
    pos = {o[0]: ALL if half is None else pl.ds(2 * half, 2), o[1]: ALL, o[2]: r}
    return tuple(pos[a] for a in AXES)


def joint(place, buf, sem):
    return remote(buf, buf, *sem, place.partner())


class Gather:
    STAGES = 6

    def __init__(self, place, ins, outs, send, recv):
        self.p, self.ins, self.outs, self.send, self.recv = place, ins, outs, send, recv

    def own(self, c, q):
        l = (q >= NTILES[c]).astype(jnp.int32)
        t = q - l * NTILES[c]
        return l, ALL, span(t, FT) if c in GU else span(t * 2 + self.p.core, LANES)

    def at(self, c, q, i):
        return self.outs[c].at[(q, *i, self.p.core) if c in GU else (q, self.p.core, *i)]

    def line(self, c, s, r):
        o = ORDER[c]
        pos = {o[0]: ALL if s else r, o[1]: r if s else self.p.at[o[1]], o[2]: self.p.at[o[2]]}
        return tuple(pos[a] for a in AXES)

    def copies(self, s, c, q):
        p, o = self.p, ORDER[c]
        sems = (self.send.at[q, c], self.recv.at[q, c, s])
        if s < 2:
            to = self.at(c, q, self.line(c, s, p.at[o[s]]))
            return [remote(to if s else self.ins[c].at[self.own(c, q)], to, *sems, p.shifted((o[s], k))) for k in (1, 2, 3)]
        if s == 4:
            half = self.at(c, q, (ALL,) * 3)
            return [remote(half, half, *sems, p.partner())]
        if s == 2:
            whole = [self.at(c, q, plane(c, p.at[o[2]]))] * 2
        else:
            whole = [self.at(c, q, plane(c, p.ring(o[2], d), h)) for h, d in enumerate((LEFT, RIGHT))]
        return [remote(whole[h], whole[h], *sems, p.shifted((o[2], d))) for h, d in enumerate((RIGHT, LEFT))]

    def joint(self, s, c, q):
        part = self.line(c, s, pl.ds(0, 3)) if s < 2 else (plane(c, pl.ds(0, 2)), plane(c, 0), (ALL,) * 3)[s - 2]
        ref = self.at(c, q, part)
        return remote(ref, ref, self.send.at[q, c], self.recv.at[q, c, s], self.p.partner())

    def keep(self, c, q):
        b = block(c, self.p)
        self.outs[c][(q, *b, self.p.core) if c in GU else (q, self.p.core, *b)] = self.ins[c][self.own(c, q)]

    def stage(self, s, c, q):
        if s > 0:
            self.joint(s - 1, c, q).wait()
        if s < 5:
            for x in self.copies(s, c, q): x.start()


def join_down(place, w_in, peer, chip):
    first = place.core == 0
    mine, other = w_in[...].astype(f32), peer[...].astype(f32)
    chip[...] = jnp.concatenate([jnp.where(first, mine, other), jnp.where(first, other, mine)], axis=1).astype(bf16)


OFFSET = (0, 1, 1)
AHEAD = 12
NEXT = 7


def fwd_kernel(x_hbm, wg_in, wu_in, wd_in, h1_hbm, g_hbm, u_hbm, at_hbm, wg0, wu0, wd0, wg1, wu1, wd1,
               x, a, act, tg, tu, td, gb, ub, atb, peer, chip, send, recv, jsem, wsem, osem, xsem):
    place = Place()
    load_x = pltpu.make_async_copy(x_hbm, x, xsem)
    load_x.start()
    place.enter(2)
    join = remote(wd_in, peer, jsem.at[0], jsem.at[1], place.partner())
    join.start()
    gather = Gather(place, (wg_in, wu_in, chip), (tg, tu, td), send, recv)

    def tick(i):
        def stages(colors):
            for s in reversed(range(Gather.STAGES)):
                for c in colors:
                    n = i // 2 - s
                    l = (n >= NEXT).astype(jnp.int32)
                    t = n - l * NEXT
                    @pl.when((t >= 0) & (t < NTILES[c]))
                    def _():
                        gather.stage(s, c, t + l * NTILES[c])
        for odd, colors in enumerate(((0,), (1, 2))):
            @pl.when(i % 2 == odd)
            def _(): stages(colors)

    def kept(l, t):
        return [pltpu.make_async_copy(v.at[t + l * NT], o.at[t], wsem.at[l, t, c]) for c, (v, o) in enumerate((((tg, wg0), (tu, wu0)), ((tg, wg1), (tu, wu1)))[l])]
    def kept_down(l, q):
        return pltpu.make_async_copy(td.at[q + l * NQ], (wd0, wd1)[l].at[q], wsem.at[l, q, DOWN])
    def out(l, t, m, s):
        r = span(m, MB)
        return [pltpu.make_async_copy(gb.at[s], g_hbm.at[l, t, r], osem.at[0, s]),
                pltpu.make_async_copy(ub.at[s], u_hbm.at[l, t, r], osem.at[1, s]),
                pltpu.make_async_copy(atb.at[s], at_hbm.at[l, span(t, FT), r], osem.at[2, s])]

    def gate_up(l, i):
        t, m, o = i // NM, i % NM, i % 2
        @pl.when(m == 0)
        def _():
            for v in kept(l, t): v.start()
        @pl.when(i >= 2)
        def _():
            for v in out(l, t, m, o): v.wait()
        am = a[span(m, MB), :]
        g = dot(am, tg[t + l * NT].reshape(D, FT))
        u = dot(am, tu[t + l * NT].reshape(D, FT))
        gb[o] = g
        ub[o] = u
        ac = (g * sigmoid(g) * u).astype(bf16)
        if l == 0:
            act[span(m, MB), span(t, FT)] = ac
        atb[o] = ac.T
        for v in out(l, t, m, o): v.start()

    def keep_all(c):
        @pl.loop(0, 2 * NTILES[c])
        def _(q): gather.keep(c, q)

    keep_all(0)
    tick(jnp.int32(0))
    keep_all(1)
    join.wait()
    join_down(place, wd_in, peer, chip)
    keep_all(DOWN)
    load_x.wait()
    rows = 2 * LANES
    @pl.loop(1, AHEAD)
    def _(i):
        tick(i)
        @pl.when(i <= T // rows)
        def _():
            r = span(i - 1, rows)
            a[r, :] = normed(x[r, :])

    @pl.loop(0, NT * NM)
    def _(i):
        t, m = i // NM, i % NM
        @pl.when((m == 0) & (t == NT - 1))
        def _():
            for q in range(NQ): kept_down(0, q).start()
        gate_up(0, i)
        @pl.when(m % 2 == 1)
        def _():
            tick(AHEAD + i // 2)

    @pl.loop(0, NM)
    def _(m):
        r = span(m, MB)
        v = dot(act[r, :], jnp.concatenate([td[j // 2, j % 2].reshape(FF, LANES) for j in range(2 * NQ)], axis=1))
        h = (x[r, :].astype(f32) + v.astype(bf16).astype(f32)).astype(bf16)
        x[r, :] = h
        a[r, :] = normed(h)
        tick(AHEAD + 2 * NT + m)
    save_h = pltpu.make_async_copy(x, h1_hbm, xsem)
    save_h.start()
    for i in (NT * NM - 2, NT * NM - 1):
        for v in out(0, i // NM, i % NM, i % 2): v.wait()

    @pl.loop(0, NT * NM)
    def _(i):
        gate_up(1, i)
        @pl.when(i % 2 == 1)
        def _():
            tick(AHEAD + 2 * NT + NM + i // 2)
    for q in range(NQ): kept_down(1, q).start()
    for i in (NT * NM - 2, NT * NM - 1):
        for v in out(1, i // NM, i % NM, i % 2): v.wait()
    for l in range(2):
        for t in range(NT):
            for v in kept(l, t): v.wait()
        for q in range(NQ): kept_down(l, q).wait()
    save_h.wait()


VM = pl.BlockSpec(memory_space=pltpu.VMEM)
ANY = pl.BlockSpec(memory_space=pl.ANY)
DMA = pltpu.SemaphoreType.DMA


def of(dtype, *shape):
    return jax.ShapeDtypeStruct(shape, dtype)


def vm(*shape, dtype=bf16):
    return pltpu.VMEM(shape, dtype)


def forward(x, *weights):
    tiles = [of(bf16, n, *tile) for n, tile in zip(NTILES, TILE)]
    return pl.pallas_call(
        fwd_kernel, name="fwd",
        out_shape=[of(bf16, T, D), of(f32, 2, NT, T, FT), of(f32, 2, NT, T, FT), of(bf16, 2, FF, T)] + tiles * 2,
        in_specs=[ANY] + [VM] * 3, out_specs=[ANY] * 10,
        scratch_shapes=[vm(T, D), vm(T, D), vm(T, FF)] + [vm(2 * n, *tile) for n, tile in zip(NTILES, TILE)] + [
            vm(2, MB, FT, dtype=f32), vm(2, MB, FT, dtype=f32), vm(2, FT, MB), vm(2, 20, D), vm(2, 40, D),
            DMA((2 * NT, 3)), DMA((2 * NT, 3, 5)), DMA((2,)), DMA((2, NT, 3)), DMA((3, 2)), DMA],
        compiler_params=pltpu.CompilerParams(collective_id=0, has_side_effects=True, vmem_limit_bytes=VMEM),
    )(x, *weights)


class Scatter:
    STAGES = 6

    def __init__(self, place, c, slots, total, tile, out, fin, sums, halves, wholes, blocks, send, recv, credit, osem):
        self.p, self.c, self.slots, self.total, self.tile, self.out, self.fin = place, c, slots, total, tile, out, fin
        self.sums, self.halves, self.wholes, self.blocks = sums, halves, wholes, blocks
        self.send, self.recv, self.credit, self.osem = send, recv, credit, osem

    def final(self, q, core):
        n = NTILES[self.c]
        l = (q < n).astype(jnp.int32)
        t = q + (l - 1) * n
        return (l, ALL, span(t, FT) if self.c in GU else span(t * 2 + core, LANES))

    def slot(self, q):
        return q % 2 if self.c in GU else q - 3 * (q * 11 // 32)

    def sem(self, q, k):
        return self.send.at[self.slot(q), k], self.recv.at[self.slot(q), k]

    def copies(self, s, q):
        p, c, n = self.p, self.c, self.slot(q)
        sem = functools.partial(self.sem, q)
        if s == 0:
            t = self.tile(q)
            return [remote(t.at[:, :, :, 1 - p.core] if c in GU else t.at[1 - p.core], self.sums.at[n], *sem(0), p.partner())]
        if s == 3:
            ways = [(k, p.in_plane(c, k, -1)) for k in PEERS]
            return [remote(self.sums.at[(n, *block(c, p, m))], self.blocks.at[n, k - 1], *sem(5), p.shifted(*m)) for k, m in ways]
        if s == 4:
            end = self.sums.at[(n, *block(c, p))]
            if c in GU:
                return [pltpu.make_async_copy(end, self.out.at[self.final(q, 0)], self.osem.at[n])]
            return [remote(end, self.fin.at[self.final(q, p.core)], *sem(6), p.partner())]
        a = ORDER[c][2]
        ways = (RIGHT, LEFT)
        if s == 1:
            two = [(self.sums.at[(n, *plane(c, p.ring(a, ACROSS), d))], self.halves.at[n, d]) for d in (0, 1)]
        else:
            two = [(self.sums.at[(n, *plane(c, p.ring(a, ways[d])))], self.wholes.at[n, d]) for d in (0, 1)]
        return [remote(*two[d], *sem(2 * s - 1 + d), p.shifted((a, ways[d]))) for d in (0, 1)]

    def add(self, i, *terms):
        v = self.sums[i].astype(f32)
        for t in terms: v = v + t.astype(f32)
        self.sums[i] = v.astype(bf16)

    def stage(self, s, q):
        p, c, n = self.p, self.c, self.slot(q)
        a = ORDER[c][2]
        if s == 4:
            joint(p, self.blocks.at[n], self.sem(q, 5)).wait()
        elif s > 0:
            for x in self.copies(s - 1, q): x.wait()
        if s == 0:
            @pl.when(q >= self.slots)
            def _():
                for i in range(18): pl.semaphore_wait(self.credit.at[i], 1)
        elif s == 1:
            t = self.tile(q)
            @pl.loop(0, 4)
            def _(x):
                self.add((n, x), t[x, :, :, p.core] if c in GU else t[p.core, x])
        elif s == 2:
            for d, way in enumerate((RIGHT, LEFT)):
                self.add((n, *plane(c, p.ring(a, way), d)), self.halves[n, d])
        elif s == 3:
            self.add((n, *plane(c, p.at[a])), self.wholes[n, 0], self.wholes[n, 1])
        elif s == 4:
            self.add((n, *block(c, p)), *(self.blocks[n, k - 1] for k in PEERS))
        else:
            if c == DOWN:
                self.fin[self.final(q, p.core)] = self.sums[(n, *block(c, p))]
            @pl.when(q < self.total - self.slots)
            def _():
                others = [p.partner(), p.shifted((a, LEFT)), p.shifted((a, RIGHT))] + [p.shifted(*p.in_plane(c, k)) for k in PEERS]
                for i, other in enumerate(others):
                    pl.semaphore_signal(self.credit.at[i], inc=1, device_id=other)
        if s < 5:
            for x in self.copies(s, q): x.start()


SLOTS = (2, 2, 3)
STEP = 6
FIRST, LATER = (1, 3, 5), (2, 4)
EVERY, DOWN_AT = 3, (0, 1, 3, 5, 7, 8)
DOWN1, DOWN0, LAST = 5, 8, 12


def bwd_kernel(h_hbm, dy_hbm, x_hbm, g_hbm, u_hbm, at_hbm, wg0, wu0, wd0, wg1, wu1, wd1,
               dx_hbm, og, ou, od,
               a, dh, at, acc, dg, du, wg, wu, wd, ob, dob, actt, gb, ub,
               wsem, gsem, dsem, xsem, *refs):
    place = Place()
    place.enter(1)
    refs = list(refs)
    take = lambda n: [refs.pop(0) for _ in range(n)]
    fin, = take(1)
    tiles = (lambda q: ob.at[q % 2, 0], lambda q: ob.at[q % 2, 1], lambda q: dob.at[q % NQ])
    outs = (og, ou, None)
    sc = []
    for c in range(3):
        sc.append(Scatter(place, c, SLOTS[c], 2 * NTILES[c], tiles[c], outs[c], fin, *take(8)))

    def weights(f, s):
        for l, (g_, u_, d_) in enumerate(((wg1, wu1, wd1), (wg0, wu0, wd0))):
            t = f - l * NT
            yield (t >= 0) & (t < NT), [pltpu.make_async_copy(g_.at[t], wg.at[s], wsem.at[0, s]), pltpu.make_async_copy(u_.at[t], wu.at[s], wsem.at[1, s])] + [
                pltpu.make_async_copy(d_.at[j // 2, j % 2, span(t, FT)], wd.at[s, :, span(j, LANES)], wsem.at[2 + j, s]) for j in range(2 * NQ)]
    def saved(i, s):
        l = (i < NT * NM).astype(jnp.int32)
        at = (l, i // NM + (l - 1) * NT, span(i % NM, MB))
        return [pltpu.make_async_copy(g_hbm.at[at], gb.at[s], gsem.at[0, s]), pltpu.make_async_copy(u_hbm.at[at], ub.at[s], gsem.at[1, s])]
    def act_in(l, t):
        return pltpu.make_async_copy(at_hbm.at[l, span(t, ROWS)], actt.at[t % 2], dsem.at[t % 2])
    def dx_out(m):
        return pltpu.make_async_copy(dh.at[span(m, MB)], dx_hbm.at[span(m, MB)], xsem.at[m])

    load_h, load_dy, load_x = (pltpu.make_async_copy(src, dst, xsem.at[i]) for i, (src, dst) in enumerate(((h_hbm, a), (dy_hbm, dh), (x_hbm, a))))
    loads = (load_h, load_dy)
    for x in loads: x.start()
    zero = jnp.int32(0)
    for x in next(weights(zero, 0))[1] + saved(zero, 0): x.start()
    for x in loads: x.wait()

    rows = 256
    @pl.loop(0, T // rows)
    def _(i):
        at[:, span(i, rows)] = normed(a[span(i, rows), :]).T

    def ff_block(f, s, m):
        r, o, i = span(m, MB), m % 2, f * NM + m
        for x in saved(i, o): x.wait()
        @pl.when(i + 1 < 2 * NT * NM)
        def _():
            for x in saved(i + 1, 1 - o): x.start()
        g, u = gb[o], ub[o]
        d = dot_t(dh[r, :], wd[s]).astype(bf16).astype(f32)
        sg = sigmoid(g)
        p = g * sg
        dgv = (d * u * (sg + p * (1 - sg))).astype(bf16)
        duv = (d * p).astype(bf16)
        dg[r, :] = dgv
        du[r, :] = duv
        acc[r, :] += dot_t(dgv, wg[s].reshape(D, FT)) + dot_t(duv, wu[s].reshape(D, FT))

    def tick(S, j):
        def gate_up(s, back):
            S0 = S - back
            @pl.when((S0 >= 0) & (S0 < LAST) & (S0 != DOWN1) & (S0 != DOWN0))
            def _():
                q = S0 - (S0 > DOWN1).astype(jnp.int32) - (S0 > DOWN0).astype(jnp.int32)
                for c in GU: sc[c].stage(s, q)
        for k, i in enumerate(LATER):
            if j == i: gate_up(1 + len(FIRST) + k, 2)
        for k, i in enumerate(FIRST):
            if j == i: gate_up(1 + k, 1)
        if j == STEP - 1: gate_up(0, 0)
        @pl.when(S > DOWN1)
        def _():
            for s in reversed(range(Scatter.STAGES)):
                if (j - DOWN_AT[s]) % EVERY == 0:
                    l = (S > DOWN0).astype(jnp.int32)
                    d = STEP // EVERY * (S - (DOWN1 + 1) - l * (DOWN0 - DOWN1)) + (j - DOWN_AT[s]) // EVERY
                    @pl.when((d >= 0) & (d < NQ))
                    def _(): sc[DOWN].stage(s, d + NQ * l)

    def block_of(S, j):
        is_down = (S == DOWN1) | (S == DOWN0)
        is_ff = (S < LAST) & (S != DOWN1) & (S != DOWN0)
        f = S - (S > DOWN1).astype(jnp.int32) - (S > DOWN0).astype(jnp.int32)
        s = f % 2
        @pl.when(is_ff & (j == 0))
        def _():
            @pl.when((f == 0) | (f == NT))
            def _():
                acc[...] = jnp.zeros_like(acc)
            for ok, copies in weights(f, s):
                @pl.when(ok)
                def _():
                    for x in copies: x.wait()
        @pl.when(is_ff & (j == STEP - 1))
        def _():
            for ok, copies in weights(f + 1, 1 - s):
                @pl.when(ok & (f + 1 < 2 * NT))
                def _():
                    for x in copies: x.start()
        @pl.when(is_ff & (j < NM))
        def _():
            ff_block(f, s, j)
        @pl.when(is_ff & (j >= NM))
        def _():
            r, x = span(j - NM, MB), pl.ds(2 * (j - NM), 2)
            for c, v in ((0, dg), (1, du)):
                ob[s, c, x] = dot(at[r, :], v[...]).reshape(2, *TILE[c][1:]).astype(bf16)
        @pl.when(is_down)
        def _():
            l = (S == DOWN1).astype(jnp.int32)
            @pl.when(j == 0)
            def _():
                act_in(l, 0).start()
                @pl.when(S == DOWN1)
                def _(): load_h.start()
            @pl.when(j < 4)
            def _():
                act_in(l, j).wait()
                @pl.when(j < 3)
                def _(): act_in(l, j + 1).start()
                v = dot(actt[j % 2], dh[...])
                for k in range(2 * NQ):
                    dob[k // 2, k % 2, j] = v[:, k * LANES:(k + 1) * LANES].reshape(4, 4, 40, LANES).astype(bf16)
            @pl.when((S == DOWN1) & (j == NT))
            def _():
                load_h.wait()
                @pl.loop(0, T // rows)
                def _(i):
                    r = span(i, rows)
                    dh[r, :] = norm_back(a[r, :], acc[r, :], dh[r, :])
                load_x.start()
                load_x.wait()
                @pl.loop(0, T // rows)
                def _(i):
                    at[:, span(i, rows)] = normed(a[span(i, rows), :]).T
        @pl.when((S == LAST) & (j < NM))
        def _():
            r = span(j, MB)
            dh[r, :] = norm_back(a[r, :], acc[r, :], dh[r, :])
            dx_out(j).start()
        for k in range(STEP):
            @pl.when(j == k)
            def _(): tick(S, k)
    @pl.loop(0, LAST + 2)
    def _(S):
        @pl.loop(0, STEP)
        def _(j): block_of(S, j)

    first = place.core == 0
    v = fin[...].astype(f32)
    od[...] = jnp.where(first, v[:, :20], v[:, 20:]).astype(bf16)
    for m in range(NM): dx_out(m).wait()


def backward(h1, dy, x, g, u, at, *tiles):
    tiles = [t if i % 3 in GU else t.reshape(NQ, 2, FF, LANES) for i, t in enumerate(tiles)]
    rings = []
    for c in range(3):
        n = SLOTS[c]
        flat = [4 // (1 + (ORDER[c][0] == x)) for x in AXES if x != ORDER[c][2]]
        rings += [vm(n, *CHIPS, *BLOCK[c]), vm(n, 2, *flat, *BLOCK[c]), vm(n, 2, 4, 4, *BLOCK[c]), vm(n, 15, *BLOCK[c]),
                  DMA((n, 7)), DMA((n, 7)), pltpu.SemaphoreType.REGULAR((18,)), DMA((n,))]
    return pl.pallas_call(
        bwd_kernel, name="bwd",
        out_shape=[of(bf16, T, D), of(bf16, 2, 8, FF), of(bf16, 2, 8, FF), of(bf16, 2, 20, D)],
        in_specs=[ANY] * 12, out_specs=[ANY] * 3 + [VM],
        scratch_shapes=[vm(T, D), vm(T, D), vm(D, T), vm(T, D, dtype=f32), vm(T, FT), vm(T, FT), vm(2, *TILE[0]), vm(2, *TILE[1]), vm(2, FT, D),
                        vm(2, 2, *TILE[0]), vm(NQ, *TILE[DOWN]), vm(2, ROWS, T), vm(2, MB, FT, dtype=f32), vm(2, MB, FT, dtype=f32),
                        DMA((10, 2)), DMA((2, 2)), DMA((2,)), DMA((NM,)), vm(2, 40, D)] + rings,
        compiler_params=pltpu.CompilerParams(collective_id=1, has_side_effects=True, vmem_limit_bytes=VMEM),
    )(h1, dy, x, g, u, at, *tiles)


def solution(mesh):
    def step(x, dy, *weights):
        h1, *saved = forward(x[0], *weights)
        dx, *grads = backward(h1, dy[0], x[0], *saved)
        return (dx[None], *grads)

    tokens, rows = P(("rep", "dp")), P(None, "dp", None)
    return jax.shard_map(step, mesh=mesh, in_specs=(tokens, tokens, rows, rows, rows), out_specs=(tokens,) + (P("rep", "dp", None),) * 3, check_vma=False)
```

```python
import functools, itertools
import jax, jax.numpy as jnp
from jax import lax
from jax.experimental import pallas as pl
from jax.experimental.pallas import tpu as pltpu
from jax.sharding import PartitionSpec as P

f32, bf16 = jnp.float32, jnp.bfloat16
T, D, FF = 2048, 1024, 2560
NT, FT = 5, 512
NQ, LANES = 4, 128
MB = 512
SUBS = 1
NM = T // MB
ROWS = FF // 4
AXES = ("x", "y", "z")
STRIDE = {"x": 32, "y": 8, "z": 2}
ORDER = (("x", "y", "z"), ("y", "z", "x"), ("z", "x", "y"))
LEFT, RIGHT, ACROSS = 3, 1, 2
GU, DOWN = (0, 1), 2
CHIPS = (4, 4, 4)
BLOCK = ((8, FT), (8, FT), (40, LANES))
TILE = ((*CHIPS, 2, *BLOCK[0]), (*CHIPS, 2, *BLOCK[1]), (2, *CHIPS, *BLOCK[DOWN]))
NTILES = (NT, NT, NQ)
VMEM = (64 << 20) - (64 << 10)
ALL = slice(None)


def dot(a, b):
    return jnp.dot(a, b, preferred_element_type=f32)


def dot_t(a, b):
    return lax.dot_general(a, b, (((1,), (1,)), ((), ())), preferred_element_type=f32)


def mult(x, n):
    return x if isinstance(x, int) else pl.multiple_of(x, n)


def span(i, n):
    return pl.ds(mult(i * n, n), n)


def sigmoid(x):
    return 0.5 * jnp.tanh(0.5 * x) + 0.5


def normed(h):
    w = h.astype(f32)
    return (w * lax.rsqrt(jnp.mean(w * w, -1, keepdims=True) + 1e-6)).astype(bf16)


def norm_back(h, da, dh):
    w = h.astype(f32)
    s = lax.rsqrt(jnp.mean(w * w, -1, keepdims=True) + 1e-6)
    d = da.astype(bf16).astype(f32)
    c = jnp.sum(d * w, -1, keepdims=True) * (s * s * s / D)
    return (dh.astype(f32) + (d * s - w * c).astype(bf16).astype(f32)).astype(bf16)


class Place:
    def __init__(self):
        self.me = lax.axis_index("dp")
        self.core = self.me % 2
        self.at = {a: self.me // STRIDE[a] % 4 for a in AXES}

    def ring(self, axis, d):
        return (self.at[axis] + d) % 4

    def shifted(self, *moves):
        return {"dp": self.me + sum((self.ring(a, d) - self.at[a]) * STRIDE[a] for a, d in moves)}

    def partner(self):
        return {"dp": self.me + 1 - 2 * self.core}

    def in_plane(self, c, k, way=1):
        return tuple(zip(ORDER[c][:2], (way * (k // 4) % 4, way * (k % 4) % 4)))

    def enter(self, still):
        barrier = pltpu.get_barrier_semaphore()
        moves = [m for m in itertools.product(range(4), repeat=3) if 3 > m.count(0) >= still]
        for m in moves:
            pl.semaphore_signal(barrier, inc=1, device_id=self.shifted(*zip(AXES, m)))
        pl.semaphore_signal(barrier, inc=1, device_id=self.partner())
        pl.semaphore_wait(barrier, len(moves) + 1)


PEERS = range(1, 16)


def remote(src, dst, send, recv, to):
    return pltpu.make_async_remote_copy(src_ref=src, dst_ref=dst, send_sem=send, recv_sem=recv, device_id=to)


def block(c, place, moves=()):
    pos = dict(moves)
    return tuple(place.ring(a, pos[a]) if a in pos else place.at[a] for a in AXES)


def plane(c, r, half=None):
    o = ORDER[c]
    pos = {o[0]: ALL if half is None else pl.ds(2 * half, 2), o[1]: ALL, o[2]: r}
    return tuple(pos[a] for a in AXES)


def joint(place, buf, sem):
    return remote(buf, buf, *sem, place.partner())


class Gather:
    STAGES = 6

    def __init__(self, place, ins, outs, send, recv):
        self.p, self.ins, self.outs, self.send, self.recv = place, ins, outs, send, recv

    def own(self, c, q):
        l = (q >= NTILES[c]).astype(jnp.int32)
        t = q - l * NTILES[c]
        return l, ALL, span(t, FT) if c in GU else span(t * 2 + self.p.core, LANES)

    def at(self, c, q, i):
        return self.outs[c].at[(q, *i, self.p.core) if c in GU else (q, self.p.core, *i)]

    def line(self, c, s, r):
        o = ORDER[c]
        pos = {o[0]: ALL if s else r, o[1]: r if s else self.p.at[o[1]], o[2]: self.p.at[o[2]]}
        return tuple(pos[a] for a in AXES)

    def copies(self, s, c, q):
        p, o = self.p, ORDER[c]
        sems = (self.send.at[q, c], self.recv.at[q, c, s])
        if s < 2:
            to = self.at(c, q, self.line(c, s, p.at[o[s]]))
            return [remote(to if s else self.ins[c].at[self.own(c, q)], to, *sems, p.shifted((o[s], k))) for k in (1, 2, 3)]
        if s == 4:
            half = self.at(c, q, (ALL,) * 3)
            return [remote(half, half, *sems, p.partner())]
        if s == 2:
            whole = [self.at(c, q, plane(c, p.at[o[2]]))] * 2
        else:
            whole = [self.at(c, q, plane(c, p.ring(o[2], d), h)) for h, d in enumerate((LEFT, RIGHT))]
        return [remote(whole[h], whole[h], *sems, p.shifted((o[2], d))) for h, d in enumerate((RIGHT, LEFT))]

    def joint(self, s, c, q):
        part = self.line(c, s, pl.ds(0, 3)) if s < 2 else (plane(c, pl.ds(0, 2)), plane(c, 0), (ALL,) * 3)[s - 2]
        ref = self.at(c, q, part)
        return remote(ref, ref, self.send.at[q, c], self.recv.at[q, c, s], self.p.partner())

    def keep(self, c, q):
        b = block(c, self.p)
        self.outs[c][(q, *b, self.p.core) if c in GU else (q, self.p.core, *b)] = self.ins[c][self.own(c, q)]

    def stage(self, s, c, q):
        if s > 0:
            self.joint(s - 1, c, q).wait()
        if s < 5:
            for x in self.copies(s, c, q): x.start()


def join_down(place, w_in, peer, chip):
    first = place.core == 0
    for l in range(2):
        mine, other = w_in[:, l, :].astype(f32), peer[:, l, :].astype(f32)
        chip[l] = jnp.concatenate([jnp.where(first, mine, other), jnp.where(first, other, mine)], axis=0).astype(bf16)


OFFSET = (0, 1, 1)
AHEAD = 12
NEXT = 7


def fwd_kernel(x_hbm, wg_in, wu_in, wd_in, h1_hbm, na_hbm, g_hbm, u_hbm, at_hbm, wg0, wu0, wd0, wg1, wu1, wd1,
               x, a, act, tg, tu, td, gb, ub, atb, nab, peer, chip, send, recv, jsem, wsem, osem, xsem, nsem):
    place = Place()
    load_x = pltpu.make_async_copy(x_hbm, x, xsem)
    load_x.start()
    place.enter(2)
    join = remote(wd_in, peer, jsem.at[0], jsem.at[1], place.partner())
    join.start()
    gather = Gather(place, (wg_in, wu_in, chip), (tg, tu, td), send, recv)

    def tick(i):
        def stages(colors):
            for s in reversed(range(Gather.STAGES)):
                for c in colors:
                    n = i // 2 - s
                    l = (n >= NEXT).astype(jnp.int32)
                    t = n - l * NEXT
                    @pl.when((t >= 0) & (t < NTILES[c]))
                    def _():
                        gather.stage(s, c, t + l * NTILES[c])
        for odd, colors in enumerate(((0,), (1, 2))):
            @pl.when(i % 2 == odd)
            def _(): stages(colors)

    def kept(l, t):
        return [pltpu.make_async_copy(v.at[t + l * NT], o.at[t], wsem.at[l, t, c]) for c, (v, o) in enumerate((((tg, wg0), (tu, wu0)), ((tg, wg1), (tu, wu1)))[l])]
    def kept_down(l, q):
        return pltpu.make_async_copy(td.at[q + l * NQ], (wd0, wd1)[l].at[q], wsem.at[l, q, DOWN])
    def out(l, t, m, s):
        r = span(m, MB)
        return [pltpu.make_async_copy(gb.at[s], g_hbm.at[l, t, r], osem.at[0, s]),
                pltpu.make_async_copy(ub.at[s], u_hbm.at[l, t, r], osem.at[1, s]),
                pltpu.make_async_copy(atb.at[s], at_hbm.at[l, span(t, FT), r], osem.at[2, s])]

    def gate_up(l, i):
        t, m, o = i // NM, i % NM, i % 2
        @pl.when(m == 0)
        def _():
            for v in kept(l, t): v.start()
        @pl.when(i >= 2)
        def _():
            for v in out(l, t, m, o): v.wait()
        am = a[span(m, MB), :]
        g = dot(am, tg[t + l * NT].reshape(D, FT))
        u = dot(am, tu[t + l * NT].reshape(D, FT))
        gb[o] = g
        ub[o] = u
        ac = (g * sigmoid(g) * u).astype(bf16)
        if l == 0:
            act[span(m, MB), span(t, FT)] = ac
        atb[o] = ac.T
        for v in out(l, t, m, o): v.start()

    def keep_all(c):
        @pl.loop(0, 2 * NTILES[c])
        def _(q): gather.keep(c, q)

    keep_all(0)
    tick(jnp.int32(0))
    keep_all(1)
    join.wait()
    join_down(place, wd_in, peer, chip)
    keep_all(DOWN)
    load_x.wait()
    rows = 2 * LANES
    def normed_out(l, i):
        return pltpu.make_async_copy(nab.at[i % 2], na_hbm.at[l, :, span(i, rows)], nsem.at[i % 2])
    def keep_normed(l, i):
        v = normed(x[span(i, rows), :])
        a[span(i, rows), :] = v
        @pl.when(i >= 2)
        def _(): normed_out(l, i).wait()
        nab[i % 2] = v.T
        normed_out(l, i).start()
    @pl.loop(1, AHEAD)
    def _(i):
        tick(i)
        @pl.when(i <= T // rows)
        def _(): keep_normed(0, i - 1)
    for i in range(2): normed_out(0, i).wait()

    @pl.loop(0, NT * NM)
    def _(i):
        t, m = i // NM, i % NM
        @pl.when((m == 0) & (t == NT - 1))
        def _():
            for q in range(NQ): kept_down(0, q).start()
        gate_up(0, i)
        @pl.when(m % 2 == 1)
        def _():
            tick(AHEAD + i // 2)

    @pl.loop(0, NM)
    def _(m):
        r = span(m, MB)
        v = dot(act[r, :], jnp.concatenate([td[j // 2, j % 2].reshape(FF, LANES) for j in range(2 * NQ)], axis=1))
        h = (x[r, :].astype(f32) + v.astype(bf16).astype(f32)).astype(bf16)
        x[r, :] = h
        for k in range(2): keep_normed(1, 2 * m + k)
        tick(AHEAD + 2 * NT + m)
    for i in range(2): normed_out(1, i).wait()
    save_h = pltpu.make_async_copy(x, h1_hbm, xsem)
    save_h.start()
    for i in (NT * NM - 2, NT * NM - 1):
        for v in out(0, i // NM, i % NM, i % 2): v.wait()

    @pl.loop(0, NT * NM)
    def _(i):
        gate_up(1, i)
        @pl.when(i % 2 == 1)
        def _():
            tick(AHEAD + 2 * NT + NM + i // 2)
    for q in range(NQ): kept_down(1, q).start()
    for i in (NT * NM - 2, NT * NM - 1):
        for v in out(1, i // NM, i % NM, i % 2): v.wait()
    for l in range(2):
        for t in range(NT):
            for v in kept(l, t): v.wait()
        for q in range(NQ): kept_down(l, q).wait()
    save_h.wait()


VM = pl.BlockSpec(memory_space=pltpu.VMEM)
ANY = pl.BlockSpec(memory_space=pl.ANY)
DMA = pltpu.SemaphoreType.DMA


def of(dtype, *shape):
    return jax.ShapeDtypeStruct(shape, dtype)


def vm(*shape, dtype=bf16):
    return pltpu.VMEM(shape, dtype)


def forward(x, *weights):
    tiles = [of(bf16, n, *tile) for n, tile in zip(NTILES, TILE)]
    return pl.pallas_call(
        fwd_kernel, name="fwd",
        out_shape=[of(bf16, T, D), of(bf16, 2, D, T), of(f32, 2, NT, T, FT), of(f32, 2, NT, T, FT), of(bf16, 2, FF, T)] + tiles * 2,
        in_specs=[ANY] + [VM] * 3, out_specs=[ANY] * 11,
        scratch_shapes=[vm(T, D), vm(T, D), vm(T, FF)] + [vm(2 * n, *tile) for n, tile in zip(NTILES, TILE)] + [
            vm(2, MB, FT, dtype=f32), vm(2, MB, FT, dtype=f32), vm(2, FT, MB), vm(2, D, 2 * LANES), vm(20, 2, D), vm(2, 40, D),
            DMA((2 * NT, 3)), DMA((2 * NT, 3, 5)), DMA((2,)), DMA((2, NT, 3)), DMA((3, 2)), DMA, DMA((2,))],
        compiler_params=pltpu.CompilerParams(collective_id=0, has_side_effects=True, vmem_limit_bytes=VMEM),
    )(x, *weights)


class Scatter:
    STAGES = 6

    def __init__(self, place, c, slots, total, tile, out, fin, sums, halves, wholes, blocks, send, recv, credit, osem):
        self.p, self.c, self.slots, self.total, self.tile, self.out, self.fin = place, c, slots, total, tile, out, fin
        self.sums, self.halves, self.wholes, self.blocks = sums, halves, wholes, blocks
        self.send, self.recv, self.credit, self.osem = send, recv, credit, osem

    def final(self, q, core):
        n = NTILES[self.c]
        l = (q < n).astype(jnp.int32)
        t = q + (l - 1) * n
        return (l, ALL, span(t, FT) if self.c in GU else span(t * 2 + core, LANES))

    def slot(self, q):
        return q % self.slots

    def sem(self, q, k):
        return self.send.at[self.slot(q), k], self.recv.at[self.slot(q), k]

    def copies(self, s, q):
        p, c, n = self.p, self.c, self.slot(q)
        sem = functools.partial(self.sem, q)
        if s == 0:
            t = self.tile(q)
            return [remote(t.at[:, :, :, 1 - p.core] if c in GU else t.at[1 - p.core], self.sums.at[n], *sem(0), p.partner())]
        if s == 3:
            ways = [(k, p.in_plane(c, k, -1)) for k in PEERS]
            return [remote(self.sums.at[(n, *block(c, p, m))], self.blocks.at[n, k - 1], *sem(5), p.shifted(*m)) for k, m in ways]
        if s == 4:
            end = self.sums.at[(n, *block(c, p))]
            if c in GU:
                return [pltpu.make_async_copy(end, self.out.at[self.final(q, 0)], self.osem.at[n])]
            return [remote(end, self.fin.at[self.final(q, p.core)], *sem(6), p.partner())]
        a = ORDER[c][2]
        ways = (RIGHT, LEFT)
        if s == 1:
            two = [(self.sums.at[(n, *plane(c, p.ring(a, ACROSS), d))], self.halves.at[n, d]) for d in (0, 1)]
        else:
            two = [(self.sums.at[(n, *plane(c, p.ring(a, ways[d])))], self.wholes.at[n, d]) for d in (0, 1)]
        return [remote(*two[d], *sem(2 * s - 1 + d), p.shifted((a, ways[d]))) for d in (0, 1)]

    def add(self, i, *terms):
        v = self.sums[i].astype(f32)
        for t in terms: v = v + t.astype(f32)
        self.sums[i] = v.astype(bf16)

    def stage(self, s, q):
        p, c, n = self.p, self.c, self.slot(q)
        a = ORDER[c][2]
        if s == 4:
            joint(p, self.blocks.at[n], self.sem(q, 5)).wait()
        elif s > 0:
            for x in self.copies(s - 1, q): x.wait()
        if s == 0:
            @pl.when(q >= self.slots)
            def _():
                for i in range(18): pl.semaphore_wait(self.credit.at[i], 1)
        elif s == 1:
            t = self.tile(q)
            @pl.loop(0, 4)
            def _(x):
                self.add((n, x), t[x, :, :, p.core] if c in GU else t[p.core, x])
        elif s == 2:
            for d, way in enumerate((RIGHT, LEFT)):
                self.add((n, *plane(c, p.ring(a, way), d)), self.halves[n, d])
        elif s == 3:
            self.add((n, *plane(c, p.at[a])), self.wholes[n, 0], self.wholes[n, 1])
        elif s == 4:
            self.add((n, *block(c, p)), *(self.blocks[n, k - 1] for k in PEERS))
        else:
            if c == DOWN:
                self.fin[self.final(q, p.core)] = self.sums[(n, *block(c, p))]
            @pl.when(q < self.total - self.slots)
            def _():
                others = [p.partner(), p.shifted((a, LEFT)), p.shifted((a, RIGHT))] + [p.shifted(*p.in_plane(c, k)) for k in PEERS]
                for i, other in enumerate(others):
                    pl.semaphore_signal(self.credit.at[i], inc=1, device_id=other)
        if s < 5:
            for x in self.copies(s, q): x.start()


SLOTS = (2, 2, 4)
STEP = 6
FIRST, LATER = (1, 3), (0, 3, 4)
EVERY, DOWN_AT = 3, (0, 1, 4, 7, 10, 11)
DOWN1, DOWN0, LAST = 5, 8, 12


def bwd_kernel(h_hbm, na_hbm, dy_hbm, x_hbm, g_hbm, u_hbm, at_hbm, wg0, wu0, wd0, wg1, wu1, wd1,
               dx_hbm, og, ou, od,
               a, dh, at, acc, dg, du, wg, wu, wd, ob, dob, actt, gb, ub,
               wsem, gsem, dsem, xsem, *refs):
    place = Place()
    place.enter(1)
    refs = list(refs)
    take = lambda n: [refs.pop(0) for _ in range(n)]
    fin, = take(1)
    tiles = (lambda q: ob.at[q % 2, 0], lambda q: ob.at[q % 2, 1], lambda q: dob.at[q % NQ])
    outs = (og, ou, None)
    sc = []
    for c in range(3):
        sc.append(Scatter(place, c, SLOTS[c], 2 * NTILES[c], tiles[c], outs[c], fin, *take(8)))

    def weights(f, s):
        for l, (g_, u_, d_) in enumerate(((wg1, wu1, wd1), (wg0, wu0, wd0))):
            t = f - l * NT
            yield (t >= 0) & (t < NT), [pltpu.make_async_copy(g_.at[t], wg.at[s], wsem.at[0, s]), pltpu.make_async_copy(u_.at[t], wu.at[s], wsem.at[1, s])] + [
                pltpu.make_async_copy(d_.at[j // 2, j % 2, span(t, FT)], wd.at[s, :, span(j, LANES)], wsem.at[2 + j, s]) for j in range(2 * NQ)]
    def saved(i, s):
        l = (i < NT * NM).astype(jnp.int32)
        at = (l, i // NM + (l - 1) * NT, span(i % NM, MB))
        return [pltpu.make_async_copy(g_hbm.at[at], gb.at[s], gsem.at[0, s]), pltpu.make_async_copy(u_hbm.at[at], ub.at[s], gsem.at[1, s])]
    def act_in(l, t):
        return pltpu.make_async_copy(at_hbm.at[l, span(t, ROWS)], actt.at[t % 2], dsem.at[t % 2])
    def dx_out(m):
        return pltpu.make_async_copy(dh.at[span(m, MB)], dx_hbm.at[span(m, MB)], xsem.at[m])

    load_h, load_dy, load_x = (pltpu.make_async_copy(src, dst, xsem.at[i]) for i, (src, dst) in enumerate(((h_hbm, a), (dy_hbm, dh), (x_hbm, a))))
    load_at = [pltpu.make_async_copy(na_hbm.at[l], at, xsem.at[NM - 1]) for l in range(2)]
    loads = (load_at[1], load_dy)
    for x in loads: x.start()
    zero = jnp.int32(0)
    for x in next(weights(zero, 0))[1] + saved(zero, 0): x.start()
    for x in loads: x.wait()

    rows = 2 * LANES
    def ff_block(f, s, m):
        r, o, i = span(m, MB), m % 2, f * NM + m
        for x in saved(i, o): x.wait()
        @pl.when(i + 1 < 2 * NT * NM)
        def _():
            for x in saved(i + 1, 1 - o): x.start()
        g, u = gb[o], ub[o]
        d = dot_t(dh[r, :], wd[s]).astype(bf16).astype(f32)
        sg = sigmoid(g)
        p = g * sg
        dgv = (d * u * (sg + p * (1 - sg))).astype(bf16)
        duv = (d * p).astype(bf16)
        dg[r, :] = dgv
        du[r, :] = duv
        acc[r, :] += dot_t(dgv, wg[s].reshape(D, FT)) + dot_t(duv, wu[s].reshape(D, FT))

    def tick(S, j):
        def gate_up(s, back):
            S0 = S - back
            @pl.when((S0 >= 0) & (S0 < LAST) & (S0 != DOWN1) & (S0 != DOWN0))
            def _():
                q = S0 - (S0 > DOWN1).astype(jnp.int32) - (S0 > DOWN0).astype(jnp.int32)
                for c in GU: sc[c].stage(s, q)
        for k, i in enumerate(LATER):
            if j == i: gate_up(1 + len(FIRST) + k, 2)
        for k, i in enumerate(FIRST):
            if j == i: gate_up(1 + k, 1)
        if j == STEP - 1: gate_up(0, 0)
        @pl.when(S > DOWN1)
        def _():
            for s in reversed(range(Scatter.STAGES)):
                if (j - DOWN_AT[s]) % EVERY == 0:
                    d = STEP // EVERY * (S - (DOWN1 + 1)) + (j - DOWN_AT[s]) // EVERY
                    gap = STEP // EVERY * (DOWN0 - DOWN1) - NQ
                    l = (d >= NQ + gap).astype(jnp.int32)
                    @pl.when((d >= 0) & (d < 2 * NQ + gap) & ((d < NQ) | (l > 0)))
                    def _(): sc[DOWN].stage(s, d - gap * l)

    def block_of(S, j):
        is_down = (S == DOWN1) | (S == DOWN0)
        is_ff = (S < LAST) & (S != DOWN1) & (S != DOWN0)
        f = S - (S > DOWN1).astype(jnp.int32) - (S > DOWN0).astype(jnp.int32)
        s = f % 2
        @pl.when(is_ff & (j == 0))
        def _():
            @pl.when((f == 0) | (f == NT))
            def _():
                acc[...] = jnp.zeros_like(acc)
            for ok, copies in weights(f, s):
                @pl.when(ok)
                def _():
                    for x in copies: x.wait()
        @pl.when(is_ff & (j == STEP - 1))
        def _():
            for ok, copies in weights(f + 1, 1 - s):
                @pl.when(ok & (f + 1 < 2 * NT))
                def _():
                    for x in copies: x.start()
        @pl.when(is_ff & (j < NM))
        def _():
            ff_block(f, s, j)
        @pl.when(is_ff & (j >= NM))
        def _():
            r, x = span(j - NM, MB), pl.ds(2 * (j - NM), 2)
            for c, v in ((0, dg), (1, du)):
                ob[s, c, x] = dot(at[r, :], v[...]).reshape(2, *TILE[c][1:]).astype(bf16)
        @pl.when(is_down)
        def _():
            l = (S == DOWN1).astype(jnp.int32)
            @pl.when(j == 0)
            def _():
                act_in(l, 0).start()
                @pl.when(S == DOWN1)
                def _():
                    load_h.start()
                    load_at[0].start()
            @pl.when(j < 4)
            def _():
                act_in(l, j).wait()
                @pl.when(j < 3)
                def _(): act_in(l, j + 1).start()
                v = dot(actt[j % 2], dh[...])
                for k in range(2 * NQ):
                    dob[k // 2, k % 2, j] = v[:, k * LANES:(k + 1) * LANES].reshape(4, 4, 40, LANES).astype(bf16)
            @pl.when((S == DOWN1) & (j == NT))
            def _():
                load_h.wait()
                @pl.loop(0, T // rows)
                def _(i):
                    r = span(i, rows)
                    dh[r, :] = norm_back(a[r, :], acc[r, :], dh[r, :])
                load_x.start()
                load_at[0].wait()
        @pl.when((S == LAST) & (j == 0))
        def _():
            load_x.wait()
        @pl.when((S == LAST) & (j < NM))
        def _():
            r = span(j, MB)
            dh[r, :] = norm_back(a[r, :], acc[r, :], dh[r, :])
            dx_out(j).start()
        for k in range(STEP):
            @pl.when(j == k)
            def _(): tick(S, k)
    @pl.loop(0, LAST + 2)
    def _(S):
        @pl.loop(0, STEP)
        def _(j): block_of(S, j)

    first = place.core == 0
    for l in range(2):
        v = fin[l].astype(f32)
        od[:, l, :] = jnp.where(first, v[:20], v[20:]).astype(bf16)
    for m in range(NM): dx_out(m).wait()


def backward(h1, normed_t, dy, x, g, u, at, *tiles):
    tiles = [t if i % 3 in GU else t.reshape(NQ, 2, FF, LANES) for i, t in enumerate(tiles)]
    rings = []
    for c in range(3):
        n = SLOTS[c]
        flat = [4 // (1 + (ORDER[c][0] == x)) for x in AXES if x != ORDER[c][2]]
        rings += [vm(n, *CHIPS, *BLOCK[c]), vm(n, 2, *flat, *BLOCK[c]), vm(n, 2, 4, 4, *BLOCK[c]), vm(n, 15, *BLOCK[c]),
                  DMA((n, 7)), DMA((n, 7)), pltpu.SemaphoreType.REGULAR((18,)), DMA((n,))]
    return pl.pallas_call(
        bwd_kernel, name="bwd",
        out_shape=[of(bf16, T, D), of(bf16, 2, 8, FF), of(bf16, 2, 8, FF), of(bf16, 20, 2, D)],
        in_specs=[ANY] * 13, out_specs=[ANY] * 3 + [VM],
        scratch_shapes=[vm(T, D), vm(T, D), vm(D, T), vm(T, D, dtype=f32), vm(T, FT), vm(T, FT), vm(2, *TILE[0]), vm(2, *TILE[1]), vm(2, FT, D),
                        vm(2, 2, *TILE[0]), vm(NQ, *TILE[DOWN]), vm(2, ROWS, T), vm(2, MB, FT, dtype=f32), vm(2, MB, FT, dtype=f32),
                        DMA((10, 2)), DMA((2, 2)), DMA((2,)), DMA((NM,)), vm(2, 40, D)] + rings,
        compiler_params=pltpu.CompilerParams(collective_id=1, has_side_effects=True, vmem_limit_bytes=VMEM),
    )(h1, normed_t, dy, x, g, u, at, *tiles)


def solution(mesh):
    def step(x, dy, *weights):
        *gate_up, down = weights
        h1, normed_t, *saved = forward(x[0], *gate_up, down.swapaxes(0, 1))
        dx, *grads, by_down = backward(h1, normed_t, dy[0], x[0], *saved)
        grads.append(by_down.swapaxes(0, 1))
        return (dx[None], *grads)

    tokens, rows = P(("rep", "dp")), P(None, "dp", None)
    return jax.shard_map(step, mesh=mesh, in_specs=(tokens, tokens, rows, rows, rows), out_specs=(tokens,) + (P("rep", "dp", None),) * 3, check_vma=False)
```

```python
import functools, itertools
import jax, jax.numpy as jnp
from jax import lax
from jax.experimental import pallas as pl
from jax.experimental.pallas import tpu as pltpu
from jax.sharding import PartitionSpec as P

f32, bf16 = jnp.float32, jnp.bfloat16
T, D, FF = 2048, 1024, 2560
NT, FT = 5, 512
NQ, LANES = 4, 128
MB = 512
SUBS = 1
NM = T // MB
ROWS = FF // 4
AXES = ("x", "y", "z")
STRIDE = {"x": 32, "y": 8, "z": 2}
ORDER = (("x", "y", "z"), ("y", "z", "x"), ("z", "x", "y"))
LEFT, RIGHT, ACROSS = 3, 1, 2
GU, DOWN = (0, 1), 2
CHIPS = (4, 4, 4)
BLOCK = ((8, FT), (8, FT), (40, LANES))
TILE = ((*CHIPS, 2, *BLOCK[0]), (*CHIPS, 2, *BLOCK[1]), (2, *CHIPS, *BLOCK[DOWN]))
NTILES = (NT, NT, NQ)
VMEM = (64 << 20) - (64 << 10)
ALL = slice(None)


def dot(a, b):
    return jnp.dot(a, b, preferred_element_type=f32)


def dot_t(a, b):
    return lax.dot_general(a, b, (((1,), (1,)), ((), ())), preferred_element_type=f32)


def mult(x, n):
    return x if isinstance(x, int) else pl.multiple_of(x, n)


def span(i, n):
    return pl.ds(mult(i * n, n), n)


def sigmoid(x):
    return 0.5 * jnp.tanh(0.5 * x) + 0.5


def normed(h):
    w = h.astype(f32)
    return (w * lax.rsqrt(jnp.mean(w * w, -1, keepdims=True) + 1e-6)).astype(bf16)


def norm_back(h, da, dh):
    w = h.astype(f32)
    s = lax.rsqrt(jnp.mean(w * w, -1, keepdims=True) + 1e-6)
    d = da.astype(bf16).astype(f32)
    c = jnp.sum(d * w, -1, keepdims=True) * (s * s * s / D)
    return (dh.astype(f32) + (d * s - w * c).astype(bf16).astype(f32)).astype(bf16)


class Place:
    def __init__(self):
        self.me = lax.axis_index("dp")
        self.core = self.me % 2
        self.at = {a: self.me // STRIDE[a] % 4 for a in AXES}

    def ring(self, axis, d):
        return (self.at[axis] + d) % 4

    def shifted(self, *moves):
        return {"dp": self.me + sum((self.ring(a, d) - self.at[a]) * STRIDE[a] for a, d in moves)}

    def partner(self):
        return {"dp": self.me + 1 - 2 * self.core}

    def in_plane(self, c, k, way=1):
        return tuple(zip(ORDER[c][:2], (way * (k // 4) % 4, way * (k % 4) % 4)))

    def enter(self, still):
        barrier = pltpu.get_barrier_semaphore()
        moves = [m for m in itertools.product(range(4), repeat=3) if 3 > m.count(0) >= still]
        for m in moves:
            pl.semaphore_signal(barrier, inc=1, device_id=self.shifted(*zip(AXES, m)))
        pl.semaphore_signal(barrier, inc=1, device_id=self.partner())
        pl.semaphore_wait(barrier, len(moves) + 1)


PEERS = range(1, 16)


def remote(src, dst, send, recv, to):
    return pltpu.make_async_remote_copy(src_ref=src, dst_ref=dst, send_sem=send, recv_sem=recv, device_id=to)


def block(c, place, moves=()):
    pos = dict(moves)
    return tuple(place.ring(a, pos[a]) if a in pos else place.at[a] for a in AXES)


def plane(c, r, half=None):
    o = ORDER[c]
    pos = {o[0]: ALL if half is None else pl.ds(2 * half, 2), o[1]: ALL, o[2]: r}
    return tuple(pos[a] for a in AXES)


def joint(place, buf, sem):
    return remote(buf, buf, *sem, place.partner())


class Gather:
    STAGES = 6

    def __init__(self, place, ins, outs, send, recv):
        self.p, self.ins, self.outs, self.send, self.recv = place, ins, outs, send, recv

    def own(self, c, q):
        l = (q >= NTILES[c]).astype(jnp.int32)
        t = q - l * NTILES[c]
        return l, ALL, span(t, FT) if c in GU else span(t * 2 + self.p.core, LANES)

    def at(self, c, q, i):
        return self.outs[c].at[(q, *i, self.p.core) if c in GU else (q, self.p.core, *i)]

    def line(self, c, s, r):
        o = ORDER[c]
        pos = {o[0]: ALL if s else r, o[1]: r if s else self.p.at[o[1]], o[2]: self.p.at[o[2]]}
        return tuple(pos[a] for a in AXES)

    def copies(self, s, c, q):
        p, o = self.p, ORDER[c]
        sems = (self.send.at[q, c], self.recv.at[q, c, s])
        if s < 2:
            to = self.at(c, q, self.line(c, s, p.at[o[s]]))
            return [remote(to if s else self.ins[c].at[self.own(c, q)], to, *sems, p.shifted((o[s], k))) for k in (1, 2, 3)]
        if s == 4:
            half = self.at(c, q, (ALL,) * 3)
            return [remote(half, half, *sems, p.partner())]
        if s == 2:
            whole = [self.at(c, q, plane(c, p.at[o[2]]))] * 2
        else:
            whole = [self.at(c, q, plane(c, p.ring(o[2], d), h)) for h, d in enumerate((LEFT, RIGHT))]
        return [remote(whole[h], whole[h], *sems, p.shifted((o[2], d))) for h, d in enumerate((RIGHT, LEFT))]

    def joint(self, s, c, q):
        part = self.line(c, s, pl.ds(0, 3)) if s < 2 else (plane(c, pl.ds(0, 2)), plane(c, 0), (ALL,) * 3)[s - 2]
        ref = self.at(c, q, part)
        return remote(ref, ref, self.send.at[q, c], self.recv.at[q, c, s], self.p.partner())

    def keep(self, c, q):
        b = block(c, self.p)
        self.outs[c][(q, *b, self.p.core) if c in GU else (q, self.p.core, *b)] = self.ins[c][self.own(c, q)]

    def stage(self, s, c, q):
        if s > 0:
            self.joint(s - 1, c, q).wait()
        if s < 5:
            for x in self.copies(s, c, q): x.start()


def join_down(place, w_in, peer, chip):
    first = place.core == 0
    for l in range(2):
        mine, other = w_in[:, l, :].astype(f32), peer[:, l, :].astype(f32)
        chip[l] = jnp.concatenate([jnp.where(first, mine, other), jnp.where(first, other, mine)], axis=0).astype(bf16)


AHEAD = 11
NEXT = 7


def fwd_kernel(x_hbm, wg_in, wu_in, wd_in, h1_hbm, na_hbm, g_hbm, u_hbm, at_hbm, wg0, wu0, wd0, wg1, wu1, wd1,
               x, a, act, tg, tu, td, gb, ub, atb, nab, peer, chip, send, recv, jsem, wsem, osem, xsem, nsem):
    place = Place()
    load_x = pltpu.make_async_copy(x_hbm, x, xsem)
    load_x.start()
    place.enter(2)
    join = remote(wd_in, peer, jsem.at[0], jsem.at[1], place.partner())
    join.start()
    gather = Gather(place, (wg_in, wu_in, chip), (tg, tu, td), send, recv)

    def tick(i):
        def stages(colors):
            for s in reversed(range(Gather.STAGES)):
                for c in colors:
                    n = i // 2 - s
                    l = (n >= NEXT).astype(jnp.int32)
                    t = n - l * NEXT
                    @pl.when((t >= 0) & (t < NTILES[c]))
                    def _():
                        gather.stage(s, c, t + l * NTILES[c])
        for odd, colors in enumerate(((0, 1), (2,))):
            @pl.when(i % 2 == odd)
            def _(): stages(colors)

    def kept(l, t):
        return [pltpu.make_async_copy(v.at[t + l * NT], o.at[t], wsem.at[l, t, c]) for c, (v, o) in enumerate((((tg, wg0), (tu, wu0)), ((tg, wg1), (tu, wu1)))[l])]
    def kept_down(l, q):
        return pltpu.make_async_copy(td.at[q + l * NQ], (wd0, wd1)[l].at[q], wsem.at[l, q, DOWN])
    def out(l, t, m, s):
        r = span(m, MB)
        return [pltpu.make_async_copy(gb.at[s], g_hbm.at[l, t, r], osem.at[0, s]),
                pltpu.make_async_copy(ub.at[s], u_hbm.at[l, t, r], osem.at[1, s]),
                pltpu.make_async_copy(atb.at[s], at_hbm.at[l, span(t, FT), r], osem.at[2, s])]

    def gate_up(l, i):
        t, m, o = i // NM, i % NM, i % 2
        @pl.when(m == 0)
        def _():
            for v in kept(l, t): v.start()
        @pl.when(i >= 2)
        def _():
            for v in out(l, t, m, o): v.wait()
        am = a[span(m, MB), :]
        g = dot(am, tg[t + l * NT].reshape(D, FT))
        u = dot(am, tu[t + l * NT].reshape(D, FT))
        gb[o] = g
        ub[o] = u
        ac = (g * sigmoid(g) * u).astype(bf16)
        if l == 0:
            act[span(m, MB), span(t, FT)] = ac
        atb[o] = ac.T
        for v in out(l, t, m, o): v.start()

    def keep_all(c):
        @pl.loop(0, 2 * NTILES[c])
        def _(q): gather.keep(c, q)

    keep_all(0)
    tick(jnp.int32(0))
    keep_all(1)
    join.wait()
    join_down(place, wd_in, peer, chip)
    keep_all(DOWN)
    load_x.wait()
    rows = 2 * LANES
    def normed_out(l, i):
        return pltpu.make_async_copy(nab.at[i % 2], na_hbm.at[l, :, span(i, rows)], nsem.at[i % 2])
    def keep_normed(l, i):
        v = normed(x[span(i, rows), :])
        a[span(i, rows), :] = v
        @pl.when(i >= 2)
        def _(): normed_out(l, i).wait()
        nab[i % 2] = v.T
        normed_out(l, i).start()
    @pl.loop(1, AHEAD)
    def _(i):
        tick(i)
        @pl.when(i <= T // rows)
        def _(): keep_normed(0, i - 1)
    for i in range(2): normed_out(0, i).wait()

    @pl.loop(0, NT * NM)
    def _(i):
        t, m = i // NM, i % NM
        @pl.when((m == 0) & (t == NT - 1))
        def _():
            for q in range(NQ): kept_down(0, q).start()
        gate_up(0, i)
        @pl.when(m % 2 == 1)
        def _():
            tick(AHEAD + i // 2)

    @pl.loop(0, NM)
    def _(m):
        r = span(m, MB)
        v = dot(act[r, :], jnp.concatenate([td[j // 2, j % 2].reshape(FF, LANES) for j in range(2 * NQ)], axis=1))
        h = (x[r, :].astype(f32) + v.astype(bf16).astype(f32)).astype(bf16)
        x[r, :] = h
        for k in range(2): keep_normed(1, 2 * m + k)
        tick(AHEAD + 2 * NT + m)
    for i in range(2): normed_out(1, i).wait()
    save_h = pltpu.make_async_copy(x, h1_hbm, xsem)
    save_h.start()
    for i in (NT * NM - 2, NT * NM - 1):
        for v in out(0, i // NM, i % NM, i % 2): v.wait()

    @pl.loop(0, NT * NM)
    def _(i):
        gate_up(1, i)
        @pl.when(i % 2 == 1)
        def _():
            tick(AHEAD + 2 * NT + NM + i // 2)
    for q in range(NQ): kept_down(1, q).start()
    for i in (NT * NM - 2, NT * NM - 1):
        for v in out(1, i // NM, i % NM, i % 2): v.wait()
    for l in range(2):
        for t in range(NT):
            for v in kept(l, t): v.wait()
        for q in range(NQ): kept_down(l, q).wait()
    save_h.wait()


VM = pl.BlockSpec(memory_space=pltpu.VMEM)
ANY = pl.BlockSpec(memory_space=pl.ANY)
DMA = pltpu.SemaphoreType.DMA


def of(dtype, *shape):
    return jax.ShapeDtypeStruct(shape, dtype)


def vm(*shape, dtype=bf16):
    return pltpu.VMEM(shape, dtype)


def forward(x, *weights):
    tiles = [of(bf16, n, *tile) for n, tile in zip(NTILES, TILE)]
    return pl.pallas_call(
        fwd_kernel, name="fwd",
        out_shape=[of(bf16, T, D), of(bf16, 2, D, T), of(f32, 2, NT, T, FT), of(f32, 2, NT, T, FT), of(bf16, 2, FF, T)] + tiles * 2,
        in_specs=[ANY] + [VM] * 3, out_specs=[ANY] * 11,
        scratch_shapes=[vm(T, D), vm(T, D), vm(T, FF)] + [vm(2 * n, *tile) for n, tile in zip(NTILES, TILE)] + [
            vm(2, MB, FT, dtype=f32), vm(2, MB, FT, dtype=f32), vm(2, FT, MB), vm(2, D, 2 * LANES), vm(20, 2, D), vm(2, 40, D),
            DMA((2 * NT, 3)), DMA((2 * NT, 3, 5)), DMA((2,)), DMA((2, NT, 3)), DMA((3, 2)), DMA, DMA((2,))],
        compiler_params=pltpu.CompilerParams(collective_id=0, has_side_effects=True, vmem_limit_bytes=VMEM),
    )(x, *weights)


class Scatter:
    STAGES = 6

    def __init__(self, place, c, slots, total, tile, out, fin, sums, halves, wholes, blocks, send, recv, credit, osem):
        self.p, self.c, self.slots, self.total, self.tile, self.out, self.fin = place, c, slots, total, tile, out, fin
        self.sums, self.halves, self.wholes, self.blocks = sums, halves, wholes, blocks
        self.send, self.recv, self.credit, self.osem = send, recv, credit, osem

    def final(self, q, core):
        n = NTILES[self.c]
        l = (q < n).astype(jnp.int32)
        t = q + (l - 1) * n
        return (l, ALL, span(t, FT) if self.c in GU else span(t * 2 + core, LANES))

    def slot(self, q):
        return q % self.slots

    def sem(self, q, k):
        return self.send.at[self.slot(q), k], self.recv.at[self.slot(q), k]

    def copies(self, s, q):
        p, c, n = self.p, self.c, self.slot(q)
        sem = functools.partial(self.sem, q)
        if s == 0:
            t = self.tile(q)
            return [remote(t.at[:, :, :, 1 - p.core] if c in GU else t.at[1 - p.core], self.sums.at[n], *sem(0), p.partner())]
        if s == 3:
            ways = [(k, p.in_plane(c, k, -1)) for k in PEERS]
            return [remote(self.sums.at[(n, *block(c, p, m))], self.blocks.at[n, k - 1], *sem(5), p.shifted(*m)) for k, m in ways]
        if s == 4:
            end = self.sums.at[(n, *block(c, p))]
            if c in GU:
                return [pltpu.make_async_copy(end, self.out.at[self.final(q, 0)], self.osem.at[n])]
            return [remote(end, self.fin.at[self.final(q, p.core)], *sem(6), p.partner())]
        a = ORDER[c][2]
        ways = (RIGHT, LEFT)
        if s == 1:
            two = [(self.sums.at[(n, *plane(c, p.ring(a, ACROSS), d))], self.halves.at[n, d]) for d in (0, 1)]
        else:
            two = [(self.sums.at[(n, *plane(c, p.ring(a, ways[d])))], self.wholes.at[n, d]) for d in (0, 1)]
        return [remote(*two[d], *sem(2 * s - 1 + d), p.shifted((a, ways[d]))) for d in (0, 1)]

    def add(self, i, *terms):
        v = self.sums[i].astype(f32)
        for t in terms: v = v + t.astype(f32)
        self.sums[i] = v.astype(bf16)

    def stage(self, s, q):
        p, c, n = self.p, self.c, self.slot(q)
        a = ORDER[c][2]
        if s == 4:
            joint(p, self.blocks.at[n], self.sem(q, 5)).wait()
        elif s > 0:
            for x in self.copies(s - 1, q): x.wait()
        if s == 0:
            @pl.when(q >= self.slots)
            def _():
                for i in range(18): pl.semaphore_wait(self.credit.at[i], 1)
        elif s == 1:
            t = self.tile(q)
            @pl.loop(0, 4)
            def _(x):
                self.add((n, x), t[x, :, :, p.core] if c in GU else t[p.core, x])
        elif s == 2:
            for d, way in enumerate((RIGHT, LEFT)):
                self.add((n, *plane(c, p.ring(a, way), d)), self.halves[n, d])
        elif s == 3:
            self.add((n, *plane(c, p.at[a])), self.wholes[n, 0], self.wholes[n, 1])
        elif s == 4:
            self.add((n, *block(c, p)), *(self.blocks[n, k - 1] for k in PEERS))
        else:
            if c == DOWN:
                self.fin[self.final(q, p.core)] = self.sums[(n, *block(c, p))]
            @pl.when(q < self.total - self.slots)
            def _():
                others = [p.partner(), p.shifted((a, LEFT)), p.shifted((a, RIGHT))] + [p.shifted(*p.in_plane(c, k)) for k in PEERS]
                for i, other in enumerate(others):
                    pl.semaphore_signal(self.credit.at[i], inc=1, device_id=other)
        if s < 5:
            for x in self.copies(s, q): x.start()


SLOTS = (2, 2, 4)
STEP = 6
FIRST, LATER = (1, 3), (0, 3, 4)
EVERY, DOWN_AT = 3, (0, 1, 4, 7, 10, 11)
DOWN1, DOWN0, LAST = 5, 8, 12


def bwd_kernel(h_hbm, na_hbm, dy_hbm, x_hbm, g_hbm, u_hbm, at_hbm, wg0, wu0, wd0, wg1, wu1, wd1,
               dx_hbm, og, ou, od,
               a, dh, at, acc, dg, du, wg, wu, wd, ob, dob, actt, gb, ub,
               wsem, gsem, dsem, xsem, *refs):
    place = Place()
    place.enter(1)
    refs = list(refs)
    take = lambda n: [refs.pop(0) for _ in range(n)]
    fin, = take(1)
    tiles = (lambda q: ob.at[q % 2, 0], lambda q: ob.at[q % 2, 1], lambda q: dob.at[q % NQ])
    outs = (og, ou, None)
    sc = []
    for c in range(3):
        sc.append(Scatter(place, c, SLOTS[c], 2 * NTILES[c], tiles[c], outs[c], fin, *take(8)))

    def weights(f, s):
        for l, (g_, u_, d_) in enumerate(((wg1, wu1, wd1), (wg0, wu0, wd0))):
            t = f - l * NT
            yield (t >= 0) & (t < NT), [pltpu.make_async_copy(g_.at[t], wg.at[s], wsem.at[0, s]), pltpu.make_async_copy(u_.at[t], wu.at[s], wsem.at[1, s])] + [
                pltpu.make_async_copy(d_.at[j // 2, j % 2, span(t, FT)], wd.at[s, :, span(j, LANES)], wsem.at[2 + j, s]) for j in range(2 * NQ)]
    def saved(i, s):
        l = (i < NT * NM).astype(jnp.int32)
        at = (l, i // NM + (l - 1) * NT, span(i % NM, MB))
        return [pltpu.make_async_copy(g_hbm.at[at], gb.at[s], gsem.at[0, s]), pltpu.make_async_copy(u_hbm.at[at], ub.at[s], gsem.at[1, s])]
    def act_in(l, t):
        return pltpu.make_async_copy(at_hbm.at[l, span(t, ROWS)], actt.at[t % 2], dsem.at[t % 2])
    def dx_out(m):
        return pltpu.make_async_copy(dh.at[span(m, MB)], dx_hbm.at[span(m, MB)], xsem.at[m])

    load_h, load_dy, load_x = (pltpu.make_async_copy(src, dst, xsem.at[i]) for i, (src, dst) in enumerate(((h_hbm, a), (dy_hbm, dh), (x_hbm, a))))
    load_at = [pltpu.make_async_copy(na_hbm.at[l], at, xsem.at[NM - 1]) for l in range(2)]
    loads = (load_at[1], load_dy)
    for x in loads: x.start()
    zero = jnp.int32(0)
    for x in next(weights(zero, 0))[1] + saved(zero, 0): x.start()
    for x in loads: x.wait()

    rows = 2 * LANES
    def ff_block(f, s, m):
        r, o, i = span(m, MB), m % 2, f * NM + m
        for x in saved(i, o): x.wait()
        @pl.when(i + 1 < 2 * NT * NM)
        def _():
            for x in saved(i + 1, 1 - o): x.start()
        g, u = gb[o], ub[o]
        d = dot_t(dh[r, :], wd[s]).astype(bf16).astype(f32)
        sg = sigmoid(g)
        p = g * sg
        dgv = (d * u * (sg + p * (1 - sg))).astype(bf16)
        duv = (d * p).astype(bf16)
        dg[r, :] = dgv
        du[r, :] = duv
        acc[r, :] += dot_t(dgv, wg[s].reshape(D, FT)) + dot_t(duv, wu[s].reshape(D, FT))

    def tick(S, j):
        def gate_up(s, back):
            S0 = S - back
            @pl.when((S0 >= 0) & (S0 < LAST) & (S0 != DOWN1) & (S0 != DOWN0))
            def _():
                q = S0 - (S0 > DOWN1).astype(jnp.int32) - (S0 > DOWN0).astype(jnp.int32)
                for c in GU: sc[c].stage(s, q)
        for k, i in enumerate(LATER):
            if j == i: gate_up(1 + len(FIRST) + k, 2)
        for k, i in enumerate(FIRST):
            if j == i: gate_up(1 + k, 1)
        if j == STEP - 1: gate_up(0, 0)
        @pl.when(S > DOWN1)
        def _():
            for s in reversed(range(Scatter.STAGES)):
                if (j - DOWN_AT[s]) % EVERY == 0:
                    d = STEP // EVERY * (S - (DOWN1 + 1)) + (j - DOWN_AT[s]) // EVERY
                    gap = STEP // EVERY * (DOWN0 - DOWN1) - NQ
                    l = (d >= NQ + gap).astype(jnp.int32)
                    @pl.when((d >= 0) & (d < 2 * NQ + gap) & ((d < NQ) | (l > 0)))
                    def _(): sc[DOWN].stage(s, d - gap * l)

    def block_of(S, j):
        is_down = (S == DOWN1) | (S == DOWN0)
        is_ff = (S < LAST) & (S != DOWN1) & (S != DOWN0)
        f = S - (S > DOWN1).astype(jnp.int32) - (S > DOWN0).astype(jnp.int32)
        s = f % 2
        @pl.when(is_ff & (j == 0))
        def _():
            @pl.when((f == 0) | (f == NT))
            def _():
                acc[...] = jnp.zeros_like(acc)
            for ok, copies in weights(f, s):
                @pl.when(ok)
                def _():
                    for x in copies: x.wait()
        @pl.when(is_ff & (j == STEP - 1))
        def _():
            for ok, copies in weights(f + 1, 1 - s):
                @pl.when(ok & (f + 1 < 2 * NT))
                def _():
                    for x in copies: x.start()
        @pl.when(is_ff & (j < NM))
        def _():
            ff_block(f, s, j)
        @pl.when(is_ff & (j >= NM))
        def _():
            r, x = span(j - NM, MB), pl.ds(2 * (j - NM), 2)
            for c, v in ((0, dg), (1, du)):
                ob[s, c, x] = dot(at[r, :], v[...]).reshape(2, *TILE[c][1:]).astype(bf16)
        @pl.when(is_down)
        def _():
            l = (S == DOWN1).astype(jnp.int32)
            @pl.when(j == 0)
            def _():
                act_in(l, 0).start()
                @pl.when(S == DOWN1)
                def _():
                    load_h.start()
                    load_at[0].start()
            @pl.when(j < 4)
            def _():
                act_in(l, j).wait()
                @pl.when(j < 3)
                def _(): act_in(l, j + 1).start()
                v = dot(actt[j % 2], dh[...])
                for k in range(2 * NQ):
                    dob[k // 2, k % 2, j] = v[:, k * LANES:(k + 1) * LANES].reshape(4, 4, 40, LANES).astype(bf16)
            @pl.when((S == DOWN1) & (j == NT))
            def _():
                load_h.wait()
                @pl.loop(0, T // rows)
                def _(i):
                    r = span(i, rows)
                    dh[r, :] = norm_back(a[r, :], acc[r, :], dh[r, :])
                load_x.start()
                load_at[0].wait()
        @pl.when((S == LAST) & (j == 0))
        def _():
            load_x.wait()
        @pl.when((S == LAST) & (j < NM))
        def _():
            r = span(j, MB)
            dh[r, :] = norm_back(a[r, :], acc[r, :], dh[r, :])
            dx_out(j).start()
        for k in range(STEP):
            @pl.when(j == k)
            def _(): tick(S, k)
    @pl.loop(0, LAST + 2)
    def _(S):
        @pl.loop(0, STEP)
        def _(j): block_of(S, j)

    first = place.core == 0
    for l in range(2):
        v = fin[l].astype(f32)
        od[:, l, :] = jnp.where(first, v[:20], v[20:]).astype(bf16)
    for m in range(NM): dx_out(m).wait()


def backward(h1, normed_t, dy, x, g, u, at, *tiles):
    tiles = [t if i % 3 in GU else t.reshape(NQ, 2, FF, LANES) for i, t in enumerate(tiles)]
    rings = []
    for c in range(3):
        n = SLOTS[c]
        flat = [4 // (1 + (ORDER[c][0] == x)) for x in AXES if x != ORDER[c][2]]
        rings += [vm(n, *CHIPS, *BLOCK[c]), vm(n, 2, *flat, *BLOCK[c]), vm(n, 2, 4, 4, *BLOCK[c]), vm(n, 15, *BLOCK[c]),
                  DMA((n, 7)), DMA((n, 7)), pltpu.SemaphoreType.REGULAR((18,)), DMA((n,))]
    return pl.pallas_call(
        bwd_kernel, name="bwd",
        out_shape=[of(bf16, T, D), of(bf16, 2, 8, FF), of(bf16, 2, 8, FF), of(bf16, 20, 2, D)],
        in_specs=[ANY] * 13, out_specs=[ANY] * 3 + [VM],
        scratch_shapes=[vm(T, D), vm(T, D), vm(D, T), vm(T, D, dtype=f32), vm(T, FT), vm(T, FT), vm(2, *TILE[0]), vm(2, *TILE[1]), vm(2, FT, D),
                        vm(2, 2, *TILE[0]), vm(NQ, *TILE[DOWN]), vm(2, ROWS, T), vm(2, MB, FT, dtype=f32), vm(2, MB, FT, dtype=f32),
                        DMA((10, 2)), DMA((2, 2)), DMA((2,)), DMA((NM,)), vm(2, 40, D)] + rings,
        compiler_params=pltpu.CompilerParams(collective_id=1, has_side_effects=True, vmem_limit_bytes=VMEM),
    )(h1, normed_t, dy, x, g, u, at, *tiles)


def solution(mesh):
    def step(x, dy, *weights):
        *gate_up, down = weights
        h1, normed_t, *saved = forward(x[0], *gate_up, down.swapaxes(0, 1))
        dx, *grads, by_down = backward(h1, normed_t, dy[0], x[0], *saved)
        grads.append(by_down.swapaxes(0, 1))
        return (dx[None], *grads)

    tokens, rows = P(("rep", "dp")), P(None, "dp", None)
    return jax.shard_map(step, mesh=mesh, in_specs=(tokens, tokens, rows, rows, rows), out_specs=(tokens,) + (P("rep", "dp", None),) * 3, check_vma=False)
```
